128 devices in a mesh: row: 16 (over x, y), col: 8 (over z, core).
Axes of the slice: x: 4, y: 4, z: 4, core: 2. Of those that a mesh axis runs over, the one named last changes fastest.
Arguments:
- fast_pos: float32 [3, 4096], P(None, ('row', 'col')), may hold values from 0 to 1
- fast_vel: float32 [3, 4096], P(None, ('row', 'col')), may hold values from -5 to 5
- fast_charge: float32 [4096], replicated, may hold values from -4 to 4
- fast_owner: int32 [4096], replicated, may hold values from 0 to 4095, as said below
- exclusions: int32 [4096, 4], replicated, may hold values from 0 to 4095, as said below
- slow_pos: float32 [3, 64, 64, 128], P(None, 'row', 'col'), may hold values from 0 to 1
- slow_vel: float32 [3, 64, 64, 128], P(None, 'row', 'col'), may hold values from -5 to 5
- slow_charge: float32 [64, 64, 128], P('row', 'col'), may hold values from -4 to 4
- neighbours: int32 [64, 64, 5], P('row', 'col'), may hold values from 0 to 24, all different within a row
Outputs:
- fast_pos_out: float32 [3, 4096], P(None, ('row', 'col'))
- fast_vel_out: float32 [3, 4096], P(None, ('row', 'col'))
- slow_pos_out: float32 [3, 64, 64, 128], P(None, 'row', 'col')
- slow_vel_out: float32 [3, 64, 64, 128], P(None, 'row', 'col')
The draws below stay inside these ranges and needn't reach their ends.
Inputs may be any that keep to these rules, and one draw needn't show every extreme that they name: `fast_owner`: atoms a and b with a % (256) == b % (256) share an owner. `exclusions`: the partners of atom a are atoms b != a with b % (256) == a % 256; a partner may repeat. `neighbours`: the entries of one cell are distinct.
All inputs are finite; a program needn't handle non-finite values.
Results may differ from the reference program's by a relative error of at most 0.0003.
Values sent between devices are 32-bit elements; how exact they have to be, the bound alone decides.
A program may use at most 64 MiB of HBM per device.

```python
import jax
import jax.numpy as jnp
from jax import lax

FAST = 4096
CELL = 128
NBR = 5
INNER = 4
OUTER = 1
CELL_ROWS = 64
CELL_COLS = 64


def draw_fast_owner(key, part):
    molecule = jax.random.randint(key, (FAST // 16,), 0, CELL_ROWS * CELL_COLS, dtype=jnp.int32)
    return jnp.tile(molecule, 16)


def draw_exclusions(key, part):
    groups = FAST // 16
    offset = jax.random.randint(key, (FAST, 4), 1, 16, dtype=jnp.int32)
    atoms = jnp.arange(FAST, dtype=jnp.int32)
    member = atoms // groups
    return (atoms % groups)[:, None] + groups * ((member[:, None] + offset) % 16)


def shard_levels(own_key, extent, split, low, high):
    level, own = 1.0, jax.random.fold_in(own_key, 6)
    for dim, blocks in split:
        heights = jnp.exp(jax.random.uniform(jax.random.fold_in(own, dim), (blocks,), jnp.float32, low / len(split), high / len(split)))
        level = level * jnp.repeat(heights, extent[dim] // blocks).reshape([-1 if axis == dim else 1 for axis in range(len(extent))])
    return level


def distinct(own_key, rows, amount, top, lift):
    ranking = jax.random.permutation(jax.random.fold_in(own_key, 1), amount)
    pull = ranking
    for power in range(3):
        pull = pull * pull // amount
    pull = pull * lift // amount
    chance = jax.random.randint(jax.random.fold_in(own_key, 2), (rows, amount), 0, 4096) + pull
    sure = jax.random.permutation(jax.random.fold_in(own_key, 3), rows)[jnp.arange(amount) % rows]
    chance = jnp.where(jnp.arange(rows)[:, None] == sure[None, :], 1 << 14, chance)
    priority = chance * amount + jnp.arange(amount)
    return lax.top_k(priority.astype(jnp.int32), top)[1].astype(jnp.int32)


def bell_draw(own_key, dims, width, limit, cuts=(), held_as=jnp.bfloat16):
    level = shard_levels(own_key, dims, cuts, -0.22, 0.18) if cuts else 1.0
    values = jax.random.normal(own_key, dims, jnp.float32) * width * level
    return jnp.minimum(jnp.maximum(values, -limit), limit).astype(held_as)


def setup_inputs(seed: int = 0) -> dict:
    seeds = jax.random.split(jax.random.key(seed), 10)
    fast_pos = jnp.clip(1.0 * jax.random.uniform(seeds[0], (3, FAST), jnp.float32) ** shard_levels(seeds[0], (3, FAST), ((1, 128),), -0.2, 0.2), 0.0, 1.0)
    fast_vel = bell_draw(seeds[1], (3, FAST), 1.0, 5.0, ((1, 128),), jnp.float32)
    fast_charge = bell_draw(seeds[2], (FAST,), 1.0, 4.0, (), jnp.float32)
    fast_owner = draw_fast_owner(jax.random.fold_in(seeds[9], 71), 0)
    exclusions = draw_exclusions(jax.random.fold_in(seeds[9], 71), 0)
    slow_pos = jnp.clip(1.0 * jax.random.uniform(seeds[5], (3, CELL_ROWS, CELL_COLS, CELL), jnp.float32) ** shard_levels(seeds[5], (3, CELL_ROWS, CELL_COLS, CELL), ((1, 16), (2, 8)), -0.2, 0.2), 0.0, 1.0)
    slow_vel = bell_draw(seeds[6], (3, CELL_ROWS, CELL_COLS, CELL), 1.0, 5.0, ((1, 16), (2, 8)), jnp.float32)
    slow_charge = bell_draw(seeds[7], (CELL_ROWS, CELL_COLS, CELL), 1.0, 4.0, ((0, 16), (1, 8)), jnp.float32)
    neighbours = distinct(seeds[8], CELL_ROWS * CELL_COLS, 25, NBR, 0).reshape((CELL_ROWS, CELL_COLS, NBR))
    return {"fast_pos": fast_pos, "fast_vel": fast_vel, "fast_charge": fast_charge, "fast_owner": fast_owner, "exclusions": exclusions, "slow_pos": slow_pos, "slow_vel": slow_vel, "slow_charge": slow_charge, "neighbours": neighbours}


fast_coupling = 1.0
slow_coupling = 0.1
outer_dt = 0.2

def owner_coords(owner, total_cols):
    grid_row = (owner // total_cols).astype(jnp.float32)
    grid_col = (owner % total_cols).astype(jnp.float32)
    return jnp.stack([grid_row, grid_col, jnp.zeros_like(grid_row)])

def pair_fast(pos_a, cell_a, charge_a, exclude_a, pos_b, cell_b, charge_b, index_b):
    delta = pos_a[:, :, None] - pos_b[:, None, :] + (cell_a[:, :, None] - cell_b[:, None, :])
    dist_sq = lax.optimization_barrier(jnp.sum(delta * delta, axis=0)) + 1.0
    inverse = 1.0 / (dist_sq * jnp.sqrt(dist_sq))
    barred = jnp.any(exclude_a[:, :, None] == index_b[None, None, :], axis=1)
    weight = jnp.where(barred, jnp.float32(0.0), charge_a[:, None] * charge_b[None, :] * inverse)
    return fast_coupling * lax.optimization_barrier(jnp.sum(weight[None] * delta, axis=2))

def slow_cells(own, views, lists):
    force = jnp.zeros((3,) + own.shape[1:], jnp.float32)
    offsets = jnp.arange(25, dtype=jnp.int32)
    for slot in range(lists.shape[-1]):
        chosen = lists[..., slot]
        pick = (chosen[..., None] == offsets).astype(jnp.float32)
        other = jnp.einsum('abo,oxabn->xabn', pick, views, precision=lax.Precision.HIGHEST)
        shift_row = (chosen // 5 - 2).astype(jnp.float32)
        shift_col = (chosen % 5 - 2).astype(jnp.float32)
        shift = jnp.stack([shift_row, shift_col, jnp.zeros_like(shift_row)])
        delta = own[0:3, :, :, :, None] - (other[0:3, :, :, None, :] + shift[:, :, :, None, None])
        dist_sq = lax.optimization_barrier(jnp.sum(delta * delta, axis=0)) + 0.5
        inverse = 1.0 / (dist_sq * jnp.sqrt(dist_sq))
        weight = other[3][:, :, None, :] * inverse
        force = force + lax.optimization_barrier(jnp.sum(weight[None] * delta, axis=-1))
    return slow_coupling * own[3][None] * force

def fast_from_cells(frac, charge, picked):
    delta = frac[:, :, None] - picked[0:3]
    dist_sq = lax.optimization_barrier(jnp.sum(delta * delta, axis=0)) + 0.5
    inverse = 1.0 / (dist_sq * jnp.sqrt(dist_sq))
    weight = picked[3] * inverse
    return slow_coupling * charge[None, :] * lax.optimization_barrier(jnp.sum(weight[None] * delta, axis=-1))

def reference(fast_pos, fast_vel, fast_charge, fast_owner, exclusions, slow_pos, slow_vel, slow_charge, neighbours):
    coords = owner_coords(fast_owner, CELL_COLS)
    all_index = jnp.arange(FAST, dtype=jnp.int32)

    def fast_force(frac):

        def one_block(start):
            pos_a = lax.dynamic_slice_in_dim(frac, start, 256, 1)
            cell_a = lax.dynamic_slice_in_dim(coords, start, 256, 1)
            charge_a = lax.dynamic_slice_in_dim(fast_charge, start, 256, 0)
            exclude_a = lax.dynamic_slice_in_dim(exclusions, start, 256, 0)
            return pair_fast(pos_a, cell_a, charge_a, exclude_a, frac, coords, fast_charge, all_index)
        starts = jnp.arange(FAST // 256, dtype=jnp.int32) * 256
        blocks = lax.map(one_block, starts)
        return jnp.transpose(blocks, (1, 0, 2)).reshape(3, FAST)
    grid_row = fast_owner // CELL_COLS
    grid_col = fast_owner % CELL_COLS

    def slow_both(spos, frac):
        data = jnp.concatenate([spos, slow_charge[None]], axis=0)
        padded = jnp.pad(data, ((0, 0), (2, 2), (2, 2), (0, 0)), mode='wrap')

        def one_row(row_start):
            slab = lax.dynamic_slice_in_dim(padded, row_start, 5, 1)
            views = jnp.stack([slab[:, o // 5:o // 5 + 1, o % 5:o % 5 + CELL_COLS] for o in range(25)])
            own = slab[:, 2:3, 2:2 + CELL_COLS]
            lists = lax.dynamic_slice_in_dim(neighbours, row_start, 1, 0)
            return slow_cells(own, views, lists)[:, 0]
        rows = lax.map(one_row, jnp.arange(CELL_ROWS, dtype=jnp.int32))
        cell_force = jnp.transpose(rows, (1, 0, 2, 3))
        picked = data[:, grid_row, grid_col, :]
        return (cell_force, fast_from_cells(frac, fast_charge, picked))
    half_outer = 0.5 * outer_dt
    inner_dt = outer_dt / INNER
    fast_acc = fast_force(fast_pos)
    slow_acc, env_acc = slow_both(slow_pos, fast_pos)
    for outer_step in range(OUTER):
        slow_vel = slow_vel + half_outer * slow_acc
        fast_vel = fast_vel + half_outer * env_acc
        for inner_step in range(INNER):
            fast_vel = fast_vel + 0.5 * inner_dt * fast_acc
            fast_pos = fast_pos + inner_dt * fast_vel
            fast_acc = fast_force(fast_pos)
            fast_vel = fast_vel + 0.5 * inner_dt * fast_acc
        slow_pos = slow_pos + outer_dt * slow_vel
        slow_acc, env_acc = slow_both(slow_pos, fast_pos)
        slow_vel = slow_vel + half_outer * slow_acc
        fast_vel = fast_vel + half_outer * env_acc
    return (fast_pos, fast_vel, slow_pos, slow_vel)
```

```python
import jax
import jax.numpy as jnp
from jax import lax
from jax.experimental import pallas as pl
from jax.experimental.pallas import tpu as pltpu
from jax.sharding import PartitionSpec as P

MESH = pl.DeviceIdType.MESH
FAST = 4096
CELL = 128
NBR = 5
INNER = 4
ROWS, COLS = 16, 8
MOL = FAST // ROWS
PIECE = MOL // COLS
CR, CC = 4, 8
CELLS = CR * CC
TOTAL_COLS = 64

fast_coupling = 1.0
slow_coupling = 0.1
outer_dt = 0.2
half_outer = 0.5 * outer_dt
inner_dt = outer_dt / INNER

SIDES = [(a, b) for a in (-1, 0, 1) for b in (-1, 0, 1) if (a, b) != (0, 0)]


def column(row):
    return jnp.transpose(jnp.broadcast_to(row, (128, 128)))


def kernel(
    own_ref, charge_ref, owner_ref, excl_ref, spos_ref, svel_ref, scharge_ref, nbr_ref,
    fpos_out, fvel_out, spos_out, svel_out,
    zrecv, gath, mat, esend, erecv, zsend2, zrecv2, acol, facc, halo_0, halo_1, scol, sacc, sforce, table, corner, barred,
    z_send, z_recv, g_send, g_recv, e_send, e_recv, y_send, y_recv, h_send, h_recv,
):
    row = lax.axis_index("row")
    col = lax.axis_index("col")
    halos = (halo_0, halo_1)
    px, py = lax.div(row, 4), lax.rem(row, 4)

    def turn(u):
        return u + lax.div(u, 2) * (5 - 2 * u)

    def peer(t):
        if isinstance(t, int):
            dx, dy = (0, 1, 3, 2)[t // 4], (0, 1, 3, 2)[t % 4]
        else:
            dx, dy = turn(lax.div(t, 4)), turn(lax.rem(t, 4))
        return lax.rem(px + dx, 4) * 4 + lax.rem(py + dy, 4)

    def line(t):
        return lax.rem(col + t, COLS)

    def side(a, b):
        return lax.rem(row + (a + ROWS), ROWS), lax.rem(col + (b + COLS), COLS)

    def remote(src, dst, send, recv, to):
        return pltpu.make_async_remote_copy(
            src_ref=src, dst_ref=dst, send_sem=send, recv_sem=recv, device_id=to, device_id_type=MESH
        )

    barrier = pltpu.get_barrier_semaphore()
    partners = [(peer(t), col) for t in range(1, ROWS)] + [(row, line(t)) for t in range(1, COLS)]
    partners += [side(a, b) for a, b in SIDES if a and b]
    for to in partners:
        pl.semaphore_signal(barrier, inc=1, device_id=to, device_id_type=MESH)

    def fill_halo(buf, pos):
        for r in range(CR):
            for comp in range(4):
                v = scharge_ref[r * CC : r * CC + CC, :] if comp == 3 else pos[comp, r * CC : r * CC + CC, :]
                for c in range(CC):
                    halos[buf][2 + r, 2 + c, comp : comp + 1, :] = v[c : c + 1, :]

    def halo_copy(buf, d):
        a, b = SIDES[d]
        rs, rd, rn = {-1: (2, 6, 2), 0: (2, 2, 4), 1: (4, 0, 2)}[a]
        cs, cd, cn = {-1: (2, 10, 2), 0: (2, 2, 8), 1: (8, 0, 2)}[b]
        return remote(
            halos[buf].at[rs : rs + rn, cs : cs + cn],
            halos[buf].at[rd : rd + rn, cd : cd + cn],
            h_send.at[buf, d],
            h_recv.at[buf, d],
            side(a, b),
        )

    def slow_columns(pos, c0, c1):
        def body(c, carry):
            for comp in range(3):
                scol[c, comp] = column(pos[comp, pl.ds(c, 1), :])
            return carry

        lax.fori_loop(c0, c1, body, 0)

    def slow_pairs(buf, c0, c1):
        def body(c, carry):
            r, k = lax.div(c, CC), lax.rem(c, CC)
            others = []
            for slot in range(NBR):
                o = nbr_ref[c, slot]
                dr = lax.div(o, 5)
                dc = o - 5 * dr
                tile = halos[buf][r + dr, k + dc]
                others.append(
                    (
                        jnp.broadcast_to(tile[0:1] + (dr - 2).astype(jnp.float32), (8, 128)),
                        jnp.broadcast_to(tile[1:2] + (dc - 2).astype(jnp.float32), (8, 128)),
                        jnp.broadcast_to(tile[2:3], (8, 128)),
                        jnp.broadcast_to(tile[3:4], (8, 128)),
                    )
                )
            for i in range(16):
                x = scol[c, 0, 8 * i : 8 * i + 8, :]
                y = scol[c, 1, 8 * i : 8 * i + 8, :]
                z = scol[c, 2, 8 * i : 8 * i + 8, :]
                fx = fy = fz = None
                for ox, oy, oz, oq in others:
                    dx, dy, dz = x - ox, y - oy, z - oz
                    s = (dx * dx + dy * dy) + (dz * dz + 0.5)
                    inv = lax.rsqrt(s)
                    w = (inv * inv) * (inv * oq)
                    if fx is None:
                        fx, fy, fz = w * dx, w * dy, w * dz
                    else:
                        fx, fy, fz = fx + w * dx, fy + w * dy, fz + w * dz
                sacc[c, 0, 8 * i : 8 * i + 8, :] = fx
                sacc[c, 1, 8 * i : 8 * i + 8, :] = fy
                sacc[c, 2, 8 * i : 8 * i + 8, :] = fz
            return carry

        lax.fori_loop(c0, c1, body, 0)

    def slow_sums(c0, c1):
        def body(c, carry):
            for comp in range(3):
                sforce[comp, pl.ds(c, 1), :] = jnp.sum(jnp.transpose(sacc[c, comp]), axis=0, keepdims=True)
            return carry

        lax.fori_loop(c0, c1, body, 0)

    def fill_table(pos):
        owner = owner_ref[...]
        gr = lax.shift_right_logical(owner, 6) - row * CR
        gc = (owner & 63) - col * CC
        inside = (gr >= 0) & (gr < CR) & (gc >= 0) & (gc < CC)
        local = jnp.where(inside, gr * CC + gc, -1)
        ids = lax.broadcasted_iota(jnp.int32, (CELLS, MOL), 0)
        pick = jnp.where(jnp.broadcast_to(local, (CELLS, MOL)) == ids, 1.0, 0.0).astype(jnp.float32)
        for comp in range(4):
            data = scharge_ref[...] if comp == 3 else pos[comp]
            table[comp * CELL : (comp + 1) * CELL, :] = jnp.dot(
                jnp.transpose(data), pick, precision=lax.Precision.HIGHEST, preferred_element_type=jnp.float32
            )

    def env_start(buf):
        mx, my, mz = mat[0], mat[1], mat[2]

        def body(jb, carry):
            fx, fy, fz = carry
            for k in range(4):
                j = jb * 4 + k
                ox, oy, oz, oq = (
                    jnp.broadcast_to(table[pl.ds(comp * CELL + j, 1), :], (ROWS, MOL)) for comp in range(4)
                )
                dx, dy, dz = mx - ox, my - oy, mz - oz
                s = (dx * dx + dy * dy) + (dz * dz + 0.5)
                inv = lax.rsqrt(s)
                w = (inv * inv) * (inv * oq)
                fx, fy, fz = fx + w * dx, fy + w * dy, fz + w * dz
            return fx, fy, fz

        zero = jnp.zeros((ROWS, MOL), jnp.float32)
        force = lax.fori_loop(0, CELL // 4, body, (zero, zero, zero))
        for r in range(ROWS):
            for comp in range(3):
                esend[buf, r, comp : comp + 1, :] = force[comp][r : r + 1, :]
            esend[buf, r, 3:4, :] = jnp.zeros((1, MOL), jnp.float32)
        for t in range(ROWS - 1, 0, -1):
            to = peer(t)
            remote(esend.at[buf, to], erecv.at[buf, row], e_send.at[buf], e_recv.at[buf], (to, col)).start()
        erecv[buf, row] = esend[buf, row]

    def env_middle(buf):
        whole = erecv.at[buf, 0 : ROWS - 1]
        remote(whole, whole, e_send.at[buf], e_recv.at[buf], (row, line(1))).wait_recv()
        total = erecv[buf, 0]
        for r in range(1, ROWS):
            total = total + erecv[buf, r]
        zsend2[buf] = total
        for t in range(COLS - 1, 0, -1):
            remote(zsend2.at[buf], zrecv2.at[buf, col], y_send.at[buf], y_recv.at[buf], (row, line(t))).start()
        zrecv2[buf, col] = total

    def env_end(buf):
        whole = zrecv2.at[buf, 0 : COLS - 1]
        remote(whole, whole, y_send.at[buf], y_recv.at[buf], (row, line(1))).wait_recv()
        total = zrecv2[buf, 0]
        for c in range(1, COLS):
            total = total + zrecv2[buf, c]
        return (slow_coupling * own_charge) * total

    def gather_start(g, pos):
        gath[g, row] = pos
        for t in range(ROWS - 1, 0, -1):
            remote(gath.at[g, row], gath.at[g, row], g_send.at[g], g_recv.at[g, row], (peer(t), col)).start()
        for comp in range(3):
            line_ = pos[comp : comp + 1, :]
            mat[comp, pl.ds(row, 1), :] = line_
            if comp < 2:
                line_ = line_ + corner[comp : comp + 1, :]
            for h in range(2):
                acol[comp, 128 * h : 128 * h + 128, :] = column(line_[:, 128 * h : 128 * h + 128])
        facc[...] = jnp.zeros_like(facc)

    def arrive(g, t):
        r = peer(t)
        slot = gath.at[g, r]
        remote(slot, slot, g_send.at[g], g_recv.at[g, r], (r, col)).wait_recv()
        for comp in range(3):
            mat[comp, pl.ds(r, 1), :] = gath[g, r, comp : comp + 1, :]

    def fast_row(g, t):
        r = peer(t)
        tile = gath[g, r]
        lines = (
            tile[0:1] + corner[0:1, :],
            tile[1:2] + corner[1:2, :],
            tile[2:3],
            charge_ref[pl.ds(r, 1), :],
        )
        halves = [[jnp.broadcast_to(v[:, 128 * h : 128 * h + 128], (8, 128)) for v in lines] for h in range(2)]
        for i in range(MOL // 8):
            x = acol[0, 8 * i : 8 * i + 8, :]
            y = acol[1, 8 * i : 8 * i + 8, :]
            z = acol[2, 8 * i : 8 * i + 8, :]
            fx = facc[0, 8 * i : 8 * i + 8, :]
            fy = facc[1, 8 * i : 8 * i + 8, :]
            fz = facc[2, 8 * i : 8 * i + 8, :]
            for ox, oy, oz, oq in halves:
                dx, dy, dz = x - ox, y - oy, z - oz
                s = (dx * dx + dy * dy) + (dz * dz + 1.0)
                inv = lax.rsqrt(s)
                w = (inv * inv) * (inv * oq)
                fx, fy, fz = fx + w * dx, fy + w * dy, fz + w * dz
            facc[0, 8 * i : 8 * i + 8, :] = fx
            facc[1, 8 * i : 8 * i + 8, :] = fy
            facc[2, 8 * i : 8 * i + 8, :] = fz

    def fast_rows(g, t0, t1, waiting):
        def body(t, carry):
            if waiting:
                arrive(g, t)
            fast_row(g, t)
            return carry

        lax.fori_loop(t0, t1, body, 0)

    def arrivals(g, t0, t1):
        def body(t, carry):
            arrive(g, t)
            return carry

        lax.fori_loop(t0, t1, body, 0)

    def fast_end(pos):
        d = [jnp.broadcast_to(pos[comp : comp + 1, :], (ROWS, MOL)) - mat[comp] for comp in range(3)]
        s = (d[0] * d[0] + d[1] * d[1]) + (d[2] * d[2] + 1.0)
        inv = lax.rsqrt(s)
        w = (inv * inv) * (inv * barred[...])
        out = []
        for comp in range(3):
            parts = [
                jnp.sum(jnp.transpose(facc[comp, 128 * h : 128 * h + 128, :]), axis=0, keepdims=True) for h in range(2)
            ]
            total = jnp.concatenate(parts, axis=1)
            out.append(total - jnp.sum(w * d[comp], axis=0, keepdims=True))
        out.append(jnp.zeros((1, MOL), jnp.float32))
        return (fast_coupling * own_charge) * jnp.concatenate(out, axis=0)

    fill_halo(0, spos_ref)
    pl.semaphore_wait(barrier, len(partners))
    for t in range(COLS - 1, 0, -1):
        remote(own_ref, zrecv.at[col], z_send, z_recv, (row, line(t))).start()
    for d in range(8):
        halo_copy(0, d).start()
    zrecv[col] = own_ref[...]
    own_charge = charge_ref[pl.ds(row, 1), :]
    owner = owner_ref[...]
    corner[0:1, :] = lax.shift_right_logical(owner, 6).astype(jnp.float32)
    corner[1:2, :] = (owner & 63).astype(jnp.float32)
    index = lax.broadcasted_iota(jnp.int32, (ROWS, MOL), 0) * MOL + lax.broadcasted_iota(jnp.int32, (ROWS, MOL), 1)
    hit = jnp.broadcast_to(excl_ref[0:1, :], (ROWS, MOL)) == index
    for e in range(1, 4):
        hit = hit | (jnp.broadcast_to(excl_ref[e : e + 1, :], (ROWS, MOL)) == index)
    barred[...] = jnp.where(hit, charge_ref[...], 0.0)
    fill_table(spos_ref)
    slow_columns(spos_ref, 0, CELLS)

    whole = zrecv.at[0 : COLS - 1]
    remote(whole, whole, z_send, z_recv, (row, line(1))).wait_recv()
    both = zrecv[0]
    for c in range(1, COLS):
        both = both + zrecv[c]
    pos, vel = both[0:4], both[4:8]

    gather_start(0, pos)
    for d in range(8):
        halo_copy(0, d).wait_recv()
    slow_pairs(0, 0, 12)
    arrivals(0, 1, ROWS)
    env_start(0)
    fast_rows(0, 0, ROWS, False)
    force = fast_end(pos)
    slow_pairs(0, 12, 18)
    env_middle(0)
    slow_pairs(0, 18, 30)
    vel = vel + half_outer * env_end(0)
    for g in range(1, INNER + 1):
        vel = vel + (0.5 * inner_dt) * force
        pos = pos + inner_dt * vel
        gather_start(g, pos)
        if g == 1:
            slow_pairs(0, 30, 32)
            slow_sums(0, CELLS)
            for comp in range(3):
                v = svel_ref[comp] + half_outer * ((slow_coupling * scharge_ref[...]) * sforce[comp])
                svel_out[comp] = v
                spos_out[comp] = spos_ref[comp] + outer_dt * v
            fill_halo(1, spos_out)
            for d in range(8):
                halo_copy(1, d).start()
        elif g == 2:
            slow_columns(spos_out, 0, CELLS)
            fill_table(spos_out)
        elif g == 3:
            for d in range(8):
                halo_copy(1, d).wait_recv()
            slow_pairs(1, 0, 8)
        else:
            slow_pairs(1, 8, 16)
        if g < INNER:
            fast_rows(g, 0, 1, False)
            fast_rows(g, 1, ROWS, True)
            force = fast_end(pos)
            vel = vel + (0.5 * inner_dt) * force
        else:
            fast_rows(g, 0, 1, False)
            fast_rows(g, 1, 12, True)
            arrivals(g, 12, ROWS)
            env_start(1)
            fast_rows(g, 12, ROWS, False)
            force = fast_end(pos)
            vel = vel + (0.5 * inner_dt) * force
    slow_pairs(1, 16, 26)
    env_middle(1)
    slow_pairs(1, 26, 32)
    slow_sums(0, CELLS)
    for comp in range(3):
        svel_out[comp] = svel_out[comp] + half_outer * ((slow_coupling * scharge_ref[...]) * sforce[comp])
    vel = vel + half_outer * env_end(1)
    back = lax.rem(MOL - col * PIECE, MOL)
    for value, out in ((pos, fpos_out), (vel, fvel_out)):
        out[...] = pltpu.roll(jnp.concatenate([value, value], axis=0), back, 1)[0:3, 0:PIECE]

    whole = zrecv.at[0 : COLS - 1]
    remote(whole, whole, z_send, z_recv, (row, line(1))).wait_send()
    for buf in range(2):
        for d in range(8):
            halo_copy(buf, d).wait_send()
        whole = erecv.at[buf, 0 : ROWS - 1]
        remote(whole, whole, e_send.at[buf], e_recv.at[buf], (row, line(1))).wait_send()
        whole = zrecv2.at[buf, 0 : COLS - 1]
        remote(whole, whole, y_send.at[buf], y_recv.at[buf], (row, line(1))).wait_send()
    for g in range(INNER + 1):
        whole = gath.at[g, 0 : ROWS - 1]
        remote(whole, whole, g_send.at[g], g_recv.at[g, 0], (row, line(1))).wait_send()


def per_device(fast_pos, fast_vel, fast_charge, fast_owner, exclusions, slow_pos, slow_vel, slow_charge, neighbours):
    row, col = lax.axis_index("row"), lax.axis_index("col")
    own = jnp.concatenate([jnp.pad(fast_pos, ((0, 1), (0, 0))), jnp.pad(fast_vel, ((0, 1), (0, 0)))], axis=0)
    own = lax.dynamic_update_slice(jnp.zeros((8, MOL), jnp.float32), own, (0, col * PIECE))
    charge = fast_charge.reshape(ROWS, MOL)
    owner = fast_owner[:MOL].reshape(1, MOL)
    excl = lax.dynamic_slice(exclusions, (row * MOL, 0), (MOL, 4)).T
    f32 = jnp.float32
    vmem = pl.BlockSpec(memory_space=pltpu.VMEM)
    dma = pltpu.SemaphoreType.DMA
    outs = pl.pallas_call(
        kernel,
        out_shape=(
            jax.ShapeDtypeStruct((3, PIECE), f32),
            jax.ShapeDtypeStruct((3, PIECE), f32),
            jax.ShapeDtypeStruct((3, CELLS, CELL), f32),
            jax.ShapeDtypeStruct((3, CELLS, CELL), f32),
        ),
        in_specs=[vmem] * 7 + [pl.BlockSpec(memory_space=pltpu.SMEM)],
        out_specs=(vmem,) * 4,
        scratch_shapes=[
            pltpu.VMEM((COLS, 8, MOL), f32),
            pltpu.VMEM((INNER + 1, ROWS, 4, MOL), f32),
            pltpu.VMEM((3, ROWS, MOL), f32),
            pltpu.VMEM((2, ROWS, 4, MOL), f32),
            pltpu.VMEM((2, ROWS, 4, MOL), f32),
            pltpu.VMEM((2, 4, MOL), f32),
            pltpu.VMEM((2, COLS, 4, MOL), f32),
            pltpu.VMEM((3, MOL, 128), f32),
            pltpu.VMEM((3, MOL, 128), f32),
            pltpu.VMEM((CR + 4, CC + 4, 4, CELL), f32),
            pltpu.VMEM((CR + 4, CC + 4, 4, CELL), f32),
            pltpu.VMEM((CELLS, 3, CELL, CELL), f32),
            pltpu.VMEM((CELLS, 3, CELL, CELL), f32),
            pltpu.VMEM((3, CELLS, CELL), f32),
            pltpu.VMEM((4 * CELL, MOL), f32),
            pltpu.VMEM((2, MOL), f32),
            pltpu.VMEM((ROWS, MOL), f32),
            dma,
            dma,
            dma((INNER + 1,)),
            dma((INNER + 1, ROWS)),
            dma((2,)),
            dma((2,)),
            dma((2,)),
            dma((2,)),
            dma((2, 8)),
            dma((2, 8)),
        ],
        compiler_params=pltpu.CompilerParams(
            collective_id=0, has_side_effects=True, vmem_limit_bytes=40 * 1024 * 1024
        ),
    )(
        own,
        charge,
        owner,
        excl,
        slow_pos.reshape(3, CELLS, CELL),
        slow_vel.reshape(3, CELLS, CELL),
        slow_charge.reshape(CELLS, CELL),
        neighbours.reshape(CELLS, NBR),
    )
    fpos, fvel, spos, svel = outs
    return fpos, fvel, spos.reshape(3, CR, CC, CELL), svel.reshape(3, CR, CC, CELL)


def solution(mesh):
    specs = (
        P(None, ("row", "col")),
        P(None, ("row", "col")),
        P(),
        P(),
        P(),
        P(None, "row", "col", None),
        P(None, "row", "col", None),
        P("row", "col", None),
        P("row", "col", None),
    )
    return jax.shard_map(
        per_device,
        mesh=mesh,
        in_specs=specs,
        out_specs=(specs[0], specs[1], specs[5], specs[6]),
        check_vma=False,
    )
```

```python
import jax
import jax.numpy as jnp
from jax import lax
from jax.experimental import pallas as pl
from jax.experimental.pallas import tpu as pltpu
from jax.sharding import PartitionSpec as P

MESH = pl.DeviceIdType.MESH
FAST = 4096
CELL = 128
NBR = 5
INNER = 4
ROWS, COLS = 16, 8
MOL = FAST // ROWS
PIECE = MOL // COLS
CR, CC = 4, 8
CELLS = CR * CC
TOTAL_COLS = 64

fast_coupling = 1.0
slow_coupling = 0.1
outer_dt = 0.2
half_outer = 0.5 * outer_dt
inner_dt = outer_dt / INNER

SIDES = [(a, b) for a in (-1, 0, 1) for b in (-1, 0, 1) if (a, b) != (0, 0)]


def column(row):
    return jnp.transpose(jnp.broadcast_to(row, (128, 128)))


def kernel(
    fpos_ref, fvel_ref, charge_ref, owner_ref, excl_ref, spos_ref, svel_ref, scharge_ref, nbr_ref,
    fpos_out, fvel_out, spos_out, svel_out,
    zrecv, gath, mat, esend, erecv, zsend2, zrecv2, acol, facc, halo_0, halo_1, scol_0, scol_1, sacc_0, sacc_1, sforce, table, zown, dsend, drecv, corner, barred,
    z_send, z_recv, g_send, g_recv, e_send, e_recv, y_send, y_recv, h_send, h_recv, d_send, d_recv,
):
    row = lax.axis_index("row")
    col = lax.axis_index("col")
    halos = (halo_0, halo_1)
    px, py = lax.div(row, 4), lax.rem(row, 4)

    def turn(u):
        return u + lax.div(u, 2) * (5 - 2 * u)

    def peer(t):
        if isinstance(t, int):
            dx, dy = (0, 1, 3, 2)[t // 4], (0, 1, 3, 2)[t % 4]
        else:
            dx, dy = turn(lax.div(t, 4)), turn(lax.rem(t, 4))
        return lax.rem(px + dx, 4) * 4 + lax.rem(py + dy, 4)

    def line(t):
        return lax.rem(col + t, COLS)

    def side(a, b):
        return lax.rem(row + (a + ROWS), ROWS), lax.rem(col + (b + COLS), COLS)

    def remote(src, dst, send, recv, to):
        return pltpu.make_async_remote_copy(
            src_ref=src, dst_ref=dst, send_sem=send, recv_sem=recv, device_id=to, device_id_type=MESH
        )

    barrier = pltpu.get_barrier_semaphore()
    partners = [(peer(t), col) for t in range(1, ROWS)] + [(row, line(t)) for t in range(1, COLS)]
    partners += [side(a, b) for a, b in SIDES if a and b]
    for to in partners:
        pl.semaphore_signal(barrier, inc=1, device_id=to, device_id_type=MESH)

    def fill_halo(buf, pos):
        for r in range(CR):
            for comp in range(4):
                v = scharge_ref[r * CC : r * CC + CC, :] if comp == 3 else pos[comp, r * CC : r * CC + CC, :]
                for c in range(CC):
                    halos[buf][2 + r, 2 + c, comp : comp + 1, :] = v[c : c + 1, :]

    def halo_copy(buf, d):
        a, b = SIDES[d]
        rs, rd, rn = {-1: (2, 6, 2), 0: (2, 2, 4), 1: (4, 0, 2)}[a]
        cs, cd, cn = {-1: (2, 10, 2), 0: (2, 2, 8), 1: (8, 0, 2)}[b]
        return remote(
            halos[buf].at[rs : rs + rn, cs : cs + cn],
            halos[buf].at[rd : rd + rn, cd : cd + cn],
            h_send.at[buf, d],
            h_recv.at[buf, d],
            side(a, b),
        )

    scols, saccs = (scol_0, scol_1), (sacc_0, sacc_1)

    def slow_columns(pos, c, into):
        for comp in range(3):
            into[comp] = column(pos[comp, pl.ds(c, 1), :])

    def slow_sums(c, acc):
        for comp in range(3):
            sforce[comp, pl.ds(c, 1), :] = jnp.sum(jnp.transpose(acc[comp]), axis=0, keepdims=True)

    def slow_cell(halo, c, scol, sacc):
        r, k = lax.div(c, CC), lax.rem(c, CC)
        others = []
        for slot in range(NBR):
            o = nbr_ref[slot, r, k]
            dr = lax.div(o, 5)
            dc = o - 5 * dr
            tile = halo[r + dr, k + dc]
            others.append(
                (
                    jnp.broadcast_to(tile[0:1] + (dr - 2).astype(jnp.float32), (8, 128)),
                    jnp.broadcast_to(tile[1:2] + (dc - 2).astype(jnp.float32), (8, 128)),
                    jnp.broadcast_to(tile[2:3], (8, 128)),
                    jnp.broadcast_to(tile[3:4], (8, 128)),
                )
            )
        for i in range(16):
            x = scol[0, 8 * i : 8 * i + 8, :]
            y = scol[1, 8 * i : 8 * i + 8, :]
            z = scol[2, 8 * i : 8 * i + 8, :]
            fx = fy = fz = None
            for ox, oy, oz, oq in others:
                dx, dy, dz = x - ox, y - oy, z - oz
                s = (dx * dx + dy * dy) + (dz * dz + 0.5)
                inv = lax.rsqrt(s)
                w = (inv * inv) * (inv * oq)
                if fx is None:
                    fx, fy, fz = w * dx, w * dy, w * dz
                else:
                    fx, fy, fz = fx + w * dx, fy + w * dy, fz + w * dz
            sacc[0, 8 * i : 8 * i + 8, :] = fx
            sacc[1, 8 * i : 8 * i + 8, :] = fy
            sacc[2, 8 * i : 8 * i + 8, :] = fz

    def slow_start(pos):
        slow_columns(pos, 0, scol_0)
        sacc_1[...] = jnp.zeros_like(sacc_1)

    def slow_pairs(buf, c0, c1):
        pos = spos_out if buf else spos_ref

        def body(p, carry):
            c = 2 * p
            slow_cell(halos[buf], c, scol_0, sacc_0)
            slow_sums(lax.max(c - 1, 0), sacc_1)
            slow_columns(pos, c + 1, scol_1)
            slow_cell(halos[buf], c + 1, scol_1, sacc_1)
            slow_sums(c, sacc_0)
            slow_columns(pos, lax.min(c + 2, CELLS - 1), scol_0)
            return carry

        lax.fori_loop(c0 // 2, c1 // 2, body, 0)

    def slow_end():
        slow_sums(CELLS - 1, sacc_1)

    def fill_table(pos):
        owner = owner_ref[0:1, :]
        gr = lax.shift_right_logical(owner, 6) - row * CR
        gc = (owner & 63) - col * CC
        inside = (gr >= 0) & (gr < CR) & (gc >= 0) & (gc < CC)
        local = jnp.where(inside, gr * CC + gc, -1)
        ids = lax.broadcasted_iota(jnp.int32, (CELLS, MOL), 0)
        pick = jnp.where(jnp.broadcast_to(local, (CELLS, MOL)) == ids, 1.0, 0.0).astype(jnp.float32)
        for comp in range(4):
            data = scharge_ref[...] if comp == 3 else pos[comp]
            table[comp * CELL : (comp + 1) * CELL, :] = jnp.dot(
                jnp.transpose(data), pick, precision=lax.Precision.HIGHEST, preferred_element_type=jnp.float32
            )

    def env_partial():
        mx, my, mz = mat[0], mat[1], mat[2]

        def body(jb, carry):
            fx, fy, fz = carry
            for k in range(4):
                j = jb * 4 + k
                ox, oy, oz, oq = (
                    jnp.broadcast_to(table[pl.ds(comp * CELL + j, 1), :], (ROWS, MOL)) for comp in range(4)
                )
                dx, dy, dz = mx - ox, my - oy, mz - oz
                s = (dx * dx + dy * dy) + (dz * dz + 0.5)
                inv = lax.rsqrt(s)
                w = (inv * inv) * (inv * oq)
                fx, fy, fz = fx + w * dx, fy + w * dy, fz + w * dz
            return fx, fy, fz

        zero = jnp.zeros((ROWS, MOL), jnp.float32)
        return lax.fori_loop(0, CELL // 4, body, (zero, zero, zero))

    def env_rows(buf):
        force = env_partial()
        for r in range(ROWS):
            for comp in range(3):
                esend[buf, r, comp : comp + 1, :] = force[comp][r : r + 1, :]
            esend[buf, r, 3:4, :] = jnp.zeros((1, MOL), jnp.float32)
        for t in range(ROWS - 1, 0, -1):
            to = peer(t)
            remote(esend.at[buf, to], erecv.at[buf, row], e_send.at[buf], e_recv.at[buf], (to, col)).start()
        erecv[buf, row] = esend[buf, row]

    def env_direct():
        force = env_partial()
        lane = lax.broadcasted_iota(jnp.int32, (ROWS, 128), 1)
        for c in range(COLS):
            h, j = c // 4, c % 4
            line_ = jnp.zeros((ROWS, 128), jnp.float32)
            for comp in range(3):
                part = force[comp][:, 128 * h : 128 * h + 128]
                shift = (32 * (comp - j)) % 128
                part = pltpu.roll(part, shift, 1) if shift else part
                line_ = jnp.where(lax.shift_right_logical(lane, 5) == comp, part, line_)
            for r in range(ROWS):
                dsend[r * COLS + c] = line_[r : r + 1, :]
        me = row * COLS + col
        for t in range(ROWS - 1, -1, -1):
            for u in range(COLS - 1, -1, -1):
                if t or u:
                    to, at = peer(t), line(u)
                    remote(dsend.at[to * COLS + at], drecv.at[me], d_send, d_recv, (to, at)).start()
        drecv[me] = dsend[me]

    def env_total():
        whole = drecv.at[0 : ROWS * COLS - 1]
        remote(whole, whole, d_send, d_recv, (row, line(1))).wait_recv()
        return jnp.sum(drecv[...], axis=0)

    def env_middle(buf):
        whole = erecv.at[buf, 0 : ROWS - 1]
        remote(whole, whole, e_send.at[buf], e_recv.at[buf], (row, line(1))).wait_recv()
        total = erecv[buf, 0]
        for r in range(1, ROWS):
            total = total + erecv[buf, r]
        zsend2[buf] = total
        for t in range(COLS - 1, 0, -1):
            remote(zsend2.at[buf], zrecv2.at[buf, col], y_send.at[buf], y_recv.at[buf], (row, line(t))).start()
        zrecv2[buf, col] = total

    def env_end(buf):
        whole = zrecv2.at[buf, 0 : COLS - 1]
        remote(whole, whole, y_send.at[buf], y_recv.at[buf], (row, line(1))).wait_recv()
        total = zrecv2[buf, 0]
        for c in range(1, COLS):
            total = total + zrecv2[buf, c]
        return (slow_coupling * own_charge) * total

    def gather_start(g, pos):
        gath[g, row] = pos
        for t in range(ROWS - 1, 0, -1):
            remote(gath.at[g, row], gath.at[g, row], g_send.at[g], g_recv.at[g, row], (peer(t), col)).start()
        for comp in range(3):
            line_ = pos[comp : comp + 1, :]
            mat[comp, pl.ds(row, 1), :] = line_
            if comp < 2:
                line_ = line_ + corner[comp : comp + 1, :]
            for h in range(2):
                acol[comp, 128 * h : 128 * h + 128, :] = column(line_[:, 128 * h : 128 * h + 128])
        facc[...] = jnp.zeros_like(facc)

    def arrive(g, t):
        r = peer(t)
        slot = gath.at[g, r]
        remote(slot, slot, g_send.at[g], g_recv.at[g, r], (r, col)).wait_recv()
        for comp in range(3):
            mat[comp, pl.ds(r, 1), :] = gath[g, r, comp : comp + 1, :]

    def fast_row(g, t):
        r = peer(t)
        tile = gath[g, r]
        lines = (
            tile[0:1] + corner[0:1, :],
            tile[1:2] + corner[1:2, :],
            tile[2:3],
            charge_ref[pl.ds(r, 1), :],
        )
        halves = [[jnp.broadcast_to(v[:, 128 * h : 128 * h + 128], (8, 128)) for v in lines] for h in range(2)]
        for i in range(MOL // 8):
            x = acol[0, 8 * i : 8 * i + 8, :]
            y = acol[1, 8 * i : 8 * i + 8, :]
            z = acol[2, 8 * i : 8 * i + 8, :]
            fx = facc[0, 8 * i : 8 * i + 8, :]
            fy = facc[1, 8 * i : 8 * i + 8, :]
            fz = facc[2, 8 * i : 8 * i + 8, :]
            for ox, oy, oz, oq in halves:
                dx, dy, dz = x - ox, y - oy, z - oz
                s = (dx * dx + dy * dy) + (dz * dz + 1.0)
                inv = lax.rsqrt(s)
                w = (inv * inv) * (inv * oq)
                fx, fy, fz = fx + w * dx, fy + w * dy, fz + w * dz
            facc[0, 8 * i : 8 * i + 8, :] = fx
            facc[1, 8 * i : 8 * i + 8, :] = fy
            facc[2, 8 * i : 8 * i + 8, :] = fz

    def fast_rows(g, t0, t1, waiting):
        def body(t, carry):
            if waiting:
                arrive(g, t)
            fast_row(g, t)
            return carry

        lax.fori_loop(t0, t1, body, 0)

    def arrivals(g, t0, t1):
        def body(t, carry):
            arrive(g, t)
            return carry

        lax.fori_loop(t0, t1, body, 0)

    def fast_end(pos):
        d = [jnp.broadcast_to(pos[comp : comp + 1, :], (ROWS, MOL)) - mat[comp] for comp in range(3)]
        s = (d[0] * d[0] + d[1] * d[1]) + (d[2] * d[2] + 1.0)
        inv = lax.rsqrt(s)
        w = (inv * inv) * (inv * barred[...])
        out = []
        for comp in range(3):
            parts = [
                jnp.sum(jnp.transpose(facc[comp, 128 * h : 128 * h + 128, :]), axis=0, keepdims=True) for h in range(2)
            ]
            total = jnp.concatenate(parts, axis=1)
            out.append(total - jnp.sum(w * d[comp], axis=0, keepdims=True))
        out.append(jnp.zeros((1, MOL), jnp.float32))
        return (fast_coupling * own_charge) * jnp.concatenate(out, axis=0)

    fill_halo(0, spos_ref)
    wide = jnp.zeros((4, MOL - PIECE), jnp.float32)
    thin = jnp.zeros((1, PIECE), jnp.float32)
    for k, ref in enumerate((fpos_ref, fvel_ref)):
        value = jnp.concatenate([jnp.concatenate([ref[...], thin], axis=0), wide], axis=1)
        zown[4 * k : 4 * k + 4, :] = pltpu.roll(jnp.concatenate([value, value], axis=0), col * PIECE, 1)[0:4]
    pl.semaphore_wait(barrier, len(partners))
    for t in range(COLS - 1, 0, -1):
        remote(zown, zrecv.at[col], z_send, z_recv, (row, line(t))).start()
    for d in range(8):
        halo_copy(0, d).start()
    zrecv[col] = zown[...]
    own_charge = charge_ref[pl.ds(row, 1), :]
    owner = owner_ref[0:1, :]
    corner[0:1, :] = lax.shift_right_logical(owner, 6).astype(jnp.float32)
    corner[1:2, :] = (owner & 63).astype(jnp.float32)
    index = lax.broadcasted_iota(jnp.int32, (ROWS, MOL), 0) * MOL + lax.broadcasted_iota(jnp.int32, (ROWS, MOL), 1)
    banned = excl_ref[:, pl.ds(pl.multiple_of(row * MOL, MOL), MOL)]
    hit = jnp.broadcast_to(banned[0:1, :], (ROWS, MOL)) == index
    for e in range(1, 4):
        hit = hit | (jnp.broadcast_to(banned[e : e + 1, :], (ROWS, MOL)) == index)
    barred[...] = jnp.where(hit, charge_ref[...], 0.0)
    fill_table(spos_ref)
    slow_start(spos_ref)

    whole = zrecv.at[0 : COLS - 1]
    remote(whole, whole, z_send, z_recv, (row, line(1))).wait_recv()
    both = zrecv[0]
    for c in range(1, COLS):
        both = both + zrecv[c]
    pos, vel = both[0:4], both[4:8]

    gather_start(0, pos)
    for d in range(8):
        halo_copy(0, d).wait_recv()
    slow_pairs(0, 0, 18)
    arrivals(0, 1, ROWS)
    env_rows(0)
    fast_rows(0, 0, ROWS, False)
    force = fast_end(pos)
    slow_pairs(0, 18, 26)
    env_middle(0)
    slow_pairs(0, 26, 32)
    slow_end()
    for comp in range(3):
        v = svel_ref[comp] + half_outer * ((slow_coupling * scharge_ref[...]) * sforce[comp])
        svel_out[comp] = v
        spos_out[comp] = spos_ref[comp] + outer_dt * v
    fill_halo(1, spos_out)
    for d in range(8):
        halo_copy(1, d).start()
    vel = vel + half_outer * env_end(0)
    for g in range(1, INNER + 1):
        vel = vel + (0.5 * inner_dt) * force
        pos = pos + inner_dt * vel
        gather_start(g, pos)
        if g == 1:
            fill_table(spos_out)
            slow_start(spos_out)
        elif g == 2:
            for d in range(8):
                halo_copy(1, d).wait_recv()
            slow_pairs(1, 0, 10)
        elif g == 3:
            slow_pairs(1, 10, 20)
        else:
            slow_pairs(1, 20, 28)
        fast_rows(g, 0, 1, False)
        if g < INNER:
            fast_rows(g, 1, ROWS, True)
            force = fast_end(pos)
            vel = vel + (0.5 * inner_dt) * force
        else:
            fast_rows(g, 1, 12, True)
            arrivals(g, 12, ROWS)
            env_direct()
            fast_rows(g, 12, ROWS, False)
            force = fast_end(pos)
            vel = vel + (0.5 * inner_dt) * force
    slow_pairs(1, 28, 32)
    slow_end()
    for comp in range(3):
        svel_out[comp] = svel_out[comp] + half_outer * ((slow_coupling * scharge_ref[...]) * sforce[comp])
    back = lax.rem(MOL - col * PIECE, MOL)

    def own_lanes(value):
        return pltpu.roll(jnp.concatenate([value, value], axis=0), back, 1)

    fpos_out[...] = own_lanes(pos)[0:3, 0:PIECE]
    vel = own_lanes(vel)
    scale = (half_outer * slow_coupling) * own_lanes(jnp.broadcast_to(own_charge, (4, MOL)))[0:1, 0:PIECE]
    total = env_total()
    for comp in range(3):
        part = pltpu.roll(jnp.broadcast_to(total, (8, 128)), 128 - 32 * comp, 1) if comp else total
        fvel_out[comp : comp + 1, :] = vel[comp : comp + 1, 0:PIECE] + scale * part[0:1, 0:PIECE]

    whole = zrecv.at[0 : COLS - 1]
    remote(whole, whole, z_send, z_recv, (row, line(1))).wait_send()
    for buf in range(2):
        for d in range(8):
            halo_copy(buf, d).wait_send()
    for ref, count, send, recv in (
        (erecv.at[0], ROWS, e_send.at[0], e_recv.at[0]),
        (zrecv2.at[0], COLS, y_send.at[0], y_recv.at[0]),
        (drecv, ROWS * COLS, d_send, d_recv),
    ):
        whole = ref.at[0 : count - 1]
        remote(whole, whole, send, recv, (row, line(1))).wait_send()
    for g in range(INNER + 1):
        whole = gath.at[g, 0 : ROWS - 1]
        remote(whole, whole, g_send.at[g], g_recv.at[g, 0], (row, line(1))).wait_send()


def finish(*refs):
    for a, b in zip(refs[:4], refs[4:]):
        b[...] = a[...]


def per_device(fast_pos, fast_vel, fast_charge, fast_owner, exclusions, slow_pos, slow_vel, slow_charge, neighbours):
    charge = fast_charge.reshape(ROWS, MOL)
    owner = fast_owner.reshape(ROWS, MOL)
    excl = exclusions.T
    f32 = jnp.float32
    vmem = pl.BlockSpec(memory_space=pltpu.VMEM)
    dma = pltpu.SemaphoreType.DMA
    outs = pl.pallas_call(
        kernel,
        out_shape=(
            jax.ShapeDtypeStruct((3, PIECE), f32),
            jax.ShapeDtypeStruct((3, PIECE), f32),
            jax.ShapeDtypeStruct((3, CELLS, CELL), f32),
            jax.ShapeDtypeStruct((3, CELLS, CELL), f32),
        ),
        in_specs=[vmem] * 8 + [pl.BlockSpec(memory_space=pltpu.SMEM)],
        out_specs=(vmem,) * 4,
        scratch_shapes=[
            pltpu.VMEM((COLS, 8, MOL), f32),
            pltpu.VMEM((INNER + 1, ROWS, 4, MOL), f32),
            pltpu.VMEM((3, ROWS, MOL), f32),
            pltpu.VMEM((2, ROWS, 4, MOL), f32),
            pltpu.VMEM((2, ROWS, 4, MOL), f32),
            pltpu.VMEM((2, 4, MOL), f32),
            pltpu.VMEM((2, COLS, 4, MOL), f32),
            pltpu.VMEM((3, MOL, 128), f32),
            pltpu.VMEM((3, MOL, 128), f32),
            pltpu.VMEM((CR + 4, CC + 4, 4, CELL), f32),
            pltpu.VMEM((CR + 4, CC + 4, 4, CELL), f32),
            pltpu.VMEM((3, CELL, CELL), f32),
            pltpu.VMEM((3, CELL, CELL), f32),
            pltpu.VMEM((3, CELL, CELL), f32),
            pltpu.VMEM((3, CELL, CELL), f32),
            pltpu.VMEM((3, CELLS, CELL), f32),
            pltpu.VMEM((4 * CELL, MOL), f32),
            pltpu.VMEM((8, MOL), f32),
            pltpu.VMEM((ROWS * COLS, 1, 128), f32),
            pltpu.VMEM((ROWS * COLS, 1, 128), f32),
            pltpu.VMEM((2, MOL), f32),
            pltpu.VMEM((ROWS, MOL), f32),
            dma,
            dma,
            dma((INNER + 1,)),
            dma((INNER + 1, ROWS)),
            dma((2,)),
            dma((2,)),
            dma((2,)),
            dma((2,)),
            dma((2, 8)),
            dma((2, 8)),
            dma,
            dma,
        ],
        compiler_params=pltpu.CompilerParams(
            collective_id=0, has_side_effects=True, vmem_limit_bytes=24 * 1024 * 1024
        ),
    )(
        fast_pos,
        fast_vel,
        charge,
        owner,
        excl,
        slow_pos.reshape(3, CELLS, CELL),
        slow_vel.reshape(3, CELLS, CELL),
        slow_charge.reshape(CELLS, CELL),
        neighbours.transpose(2, 0, 1),
    )
    outs = pl.pallas_call(
        finish, out_shape=[jax.ShapeDtypeStruct(o.shape, f32) for o in outs], in_specs=[vmem] * 4, out_specs=[vmem] * 4
    )(*outs)
    fpos, fvel, spos, svel = outs
    return fpos, fvel, spos.reshape(3, CR, CC, CELL), svel.reshape(3, CR, CC, CELL)


def solution(mesh):
    specs = (
        P(None, ("row", "col")),
        P(None, ("row", "col")),
        P(),
        P(),
        P(),
        P(None, "row", "col", None),
        P(None, "row", "col", None),
        P("row", "col", None),
        P("row", "col", None),
    )
    return jax.shard_map(
        per_device,
        mesh=mesh,
        in_specs=specs,
        out_specs=(specs[0], specs[1], specs[5], specs[6]),
        check_vma=False,
    )
```

```python
import jax
import jax.numpy as jnp
from jax import lax
from jax.experimental import pallas as pl
from jax.experimental.pallas import tpu as pltpu
from jax.sharding import PartitionSpec as P

MESH = pl.DeviceIdType.MESH
FAST = 4096
CELL = 128
NBR = 5
INNER = 4
ROWS, COLS = 16, 8
MOL = FAST // ROWS
PIECE = MOL // COLS
CR, CC = 4, 8
CELLS = CR * CC
VMEM = 67043328

ORDER = (0, 1, 3, 4, 12, 2, 8, 5, 7, 13, 15, 6, 14, 9, 11, 10)

fast_coupling = 1.0
slow_coupling = 0.1
outer_dt = 0.2
half_outer = 0.5 * outer_dt
inner_dt = outer_dt / INNER

SIDES = [(a, b) for a in (-1, 0, 1) for b in (-1, 0, 1) if (a, b) != (0, 0)]


def column(row):
    return jnp.transpose(jnp.broadcast_to(row, (128, 128)))


def kernel(
    fpos_in, fvel_in, charge_in, owner_in, excl_in, spos_in, svel_in, scharge_in, nbr_in,
    fpos_out, fvel_out, spos_out, svel_out,
    fpos_ref, fvel_ref, charge_raw, owner_ref, excl_ref, spos_ref, svel_ref, scharge_ref, nbr_ref, charge_ref, in_sem,
    zrecv, gath, mat, esend, erecv, zsend2, zrecv2, acol, facc, halo_0, halo_1, scol_0, scol_1, sacc_0, sacc_1, sforce, table, zown, dsend, drecv, corner, barred,
    z_send, z_recv, g_send, g_recv, e_send, e_recv, y_send, y_recv, h_send, h_recv, d_send, d_recv,
):
    row = lax.axis_index("row")
    col = lax.axis_index("col")
    halos = (halo_0, halo_1)
    px, py = lax.div(row, 4), lax.rem(row, 4)

    def peer(t):
        if isinstance(t, int):
            code = ORDER[t]
            dx, dy = code // 4, code % 4
        else:
            code = jnp.int32(0)
            for k in range(1, ROWS):
                code = jnp.where(t == k, ORDER[k], code)
            dx, dy = lax.div(code, 4), lax.rem(code, 4)
        return lax.rem(px + dx, 4) * 4 + lax.rem(py + dy, 4)

    def line(t):
        return lax.rem(col + t, COLS)

    def side(a, b):
        return lax.rem(row + (a + ROWS), ROWS), lax.rem(col + (b + COLS), COLS)

    def remote(src, dst, send, recv, to):
        return pltpu.make_async_remote_copy(
            src_ref=src, dst_ref=dst, send_sem=send, recv_sem=recv, device_id=to, device_id_type=MESH
        )

    loads = [
        pltpu.make_async_copy(src, dst, in_sem.at[k])
        for k, (src, dst) in enumerate(
            (
                (spos_in, spos_ref),
                (scharge_in, scharge_ref),
                (fpos_in, fpos_ref),
                (fvel_in, fvel_ref),
                (charge_in, charge_raw),
                (owner_in.at[0:8], owner_ref),
                (excl_in.at[:, pl.ds(pl.multiple_of(row * MOL, MOL), MOL)], excl_ref),
                (nbr_in, nbr_ref),
                (svel_in, svel_ref),
            )
        )
    ]
    for load in loads:
        load.start()

    barrier = pltpu.get_barrier_semaphore()
    partners = [(peer(t), col) for t in range(1, ROWS)] + [(row, line(t)) for t in range(1, COLS)]
    partners += [side(a, b) for a, b in SIDES if a and b]
    for to in partners:
        pl.semaphore_signal(barrier, inc=1, device_id=to, device_id_type=MESH)

    def fill_halo(buf, pos):
        for r in range(CR):
            for comp in range(4):
                v = scharge_ref[r * CC : r * CC + CC, :] if comp == 3 else pos[comp, r * CC : r * CC + CC, :]
                for c in range(CC):
                    halos[buf][2 + r, 2 + c, comp : comp + 1, :] = v[c : c + 1, :]

    def halo_copy(buf, d):
        a, b = SIDES[d]
        rs, rd, rn = {-1: (2, 6, 2), 0: (2, 2, 4), 1: (4, 0, 2)}[a]
        cs, cd, cn = {-1: (2, 10, 2), 0: (2, 2, 8), 1: (8, 0, 2)}[b]
        return remote(
            halos[buf].at[rs : rs + rn, cs : cs + cn],
            halos[buf].at[rd : rd + rn, cd : cd + cn],
            h_send.at[buf, d],
            h_recv.at[buf, d],
            side(a, b),
        )

    scols, saccs = (scol_0, scol_1), (sacc_0, sacc_1)

    def slow_columns(pos, c, into):
        for comp in range(3):
            into[comp] = column(pos[comp, pl.ds(c, 1), :])

    def slow_sums(c, acc):
        for comp in range(3):
            sforce[comp, pl.ds(c, 1), :] = jnp.sum(jnp.transpose(acc[comp]), axis=0, keepdims=True)

    def slow_cell(halo, c, scol, sacc):
        r, k = lax.div(c, CC), lax.rem(c, CC)
        others = []
        for slot in range(NBR):
            o = nbr_ref[slot, r, k]
            dr = lax.div(o, 5)
            dc = o - 5 * dr
            tile = halo[r + dr, k + dc]
            others.append(
                (
                    jnp.broadcast_to(tile[0:1] + (dr - 2).astype(jnp.float32), (8, 128)),
                    jnp.broadcast_to(tile[1:2] + (dc - 2).astype(jnp.float32), (8, 128)),
                    jnp.broadcast_to(tile[2:3], (8, 128)),
                    jnp.broadcast_to(tile[3:4], (8, 128)),
                )
            )
        for i in range(16):
            x = scol[0, 8 * i : 8 * i + 8, :]
            y = scol[1, 8 * i : 8 * i + 8, :]
            z = scol[2, 8 * i : 8 * i + 8, :]
            fx = fy = fz = None
            for ox, oy, oz, oq in others:
                dx, dy, dz = x - ox, y - oy, z - oz
                s = (dx * dx + dy * dy) + (dz * dz + 0.5)
                inv = lax.rsqrt(s)
                w = (inv * inv) * (inv * oq)
                if fx is None:
                    fx, fy, fz = w * dx, w * dy, w * dz
                else:
                    fx, fy, fz = fx + w * dx, fy + w * dy, fz + w * dz
            sacc[0, 8 * i : 8 * i + 8, :] = fx
            sacc[1, 8 * i : 8 * i + 8, :] = fy
            sacc[2, 8 * i : 8 * i + 8, :] = fz

    def slow_start(pos):
        slow_columns(pos, 0, scol_0)
        sacc_1[...] = jnp.zeros_like(sacc_1)

    def slow_pairs(buf, c0, c1):
        pos = spos_out if buf else spos_ref

        def body(p, carry):
            c = 2 * p
            slow_cell(halos[buf], c, scol_0, sacc_0)
            slow_sums(lax.max(c - 1, 0), sacc_1)
            slow_columns(pos, c + 1, scol_1)
            slow_cell(halos[buf], c + 1, scol_1, sacc_1)
            slow_sums(c, sacc_0)
            slow_columns(pos, lax.min(c + 2, CELLS - 1), scol_0)
            return carry

        lax.fori_loop(c0 // 2, c1 // 2, body, 0)

    def slow_end():
        slow_sums(CELLS - 1, sacc_1)

    def owner_line():
        return jnp.concatenate([owner_ref[0:1, :], owner_ref[1:2, :]], axis=1)

    def fill_table(pos):
        owner = owner_line()
        gr = lax.shift_right_logical(owner, 6) - row * CR
        gc = (owner & 63) - col * CC
        inside = (gr >= 0) & (gr < CR) & (gc >= 0) & (gc < CC)
        local = jnp.where(inside, gr * CC + gc, -1)
        ids = lax.broadcasted_iota(jnp.int32, (CELLS, MOL), 0)
        pick = jnp.where(jnp.broadcast_to(local, (CELLS, MOL)) == ids, 1.0, 0.0).astype(jnp.float32)
        for comp in range(4):
            data = scharge_ref[...] if comp == 3 else pos[comp]
            table[comp * CELL : (comp + 1) * CELL, :] = jnp.dot(
                jnp.transpose(data), pick, precision=lax.Precision.HIGHEST, preferred_element_type=jnp.float32
            )

    def env_partial():
        mx, my, mz = mat[0], mat[1], mat[2]

        def body(jb, carry):
            fx, fy, fz = carry
            for k in range(4):
                j = jb * 4 + k
                ox, oy, oz, oq = (
                    jnp.broadcast_to(table[pl.ds(comp * CELL + j, 1), :], (ROWS, MOL)) for comp in range(4)
                )
                dx, dy, dz = mx - ox, my - oy, mz - oz
                s = (dx * dx + dy * dy) + (dz * dz + 0.5)
                inv = lax.rsqrt(s)
                w = (inv * inv) * (inv * oq)
                fx, fy, fz = fx + w * dx, fy + w * dy, fz + w * dz
            return fx, fy, fz

        zero = jnp.zeros((ROWS, MOL), jnp.float32)
        return lax.fori_loop(0, CELL // 4, body, (zero, zero, zero))

    def env_rows(buf):
        force = env_partial()
        for r in range(ROWS):
            for comp in range(3):
                esend[buf, r, comp : comp + 1, :] = force[comp][r : r + 1, :]
            esend[buf, r, 3:4, :] = jnp.zeros((1, MOL), jnp.float32)
        for t in range(ROWS - 1, 0, -1):
            to = peer(t)
            remote(esend.at[buf, to], erecv.at[buf, row], e_send.at[buf], e_recv.at[buf], (to, col)).start()
        erecv[buf, row] = esend[buf, row]

    def env_direct():
        force = env_partial()
        lane = lax.broadcasted_iota(jnp.int32, (ROWS, 128), 1)
        for c in range(COLS):
            h, j = c // 4, c % 4
            line_ = jnp.zeros((ROWS, 128), jnp.float32)
            for comp in range(3):
                part = force[comp][:, 128 * h : 128 * h + 128]
                shift = (32 * (comp - j)) % 128
                part = pltpu.roll(part, shift, 1) if shift else part
                line_ = jnp.where(lax.shift_right_logical(lane, 5) == comp, part, line_)
            for r in range(ROWS):
                dsend[r * COLS + c] = line_[r : r + 1, :]
        me = row * COLS + col
        for t in range(ROWS - 1, -1, -1):
            for u in range(COLS - 1, -1, -1):
                if t or u:
                    to, at = peer(t), line(u)
                    remote(dsend.at[to * COLS + at], drecv.at[me], d_send, d_recv, (to, at)).start()
        drecv[me] = dsend[me]

    def env_total():
        whole = drecv.at[0 : ROWS * COLS - 1]
        remote(whole, whole, d_send, d_recv, (row, line(1))).wait_recv()
        return jnp.sum(drecv[...], axis=0)

    def env_middle(buf):
        whole = erecv.at[buf, 0 : ROWS - 1]
        remote(whole, whole, e_send.at[buf], e_recv.at[buf], (row, line(1))).wait_recv()
        total = erecv[buf, 0]
        for r in range(1, ROWS):
            total = total + erecv[buf, r]
        zsend2[buf] = total
        for t in range(COLS - 1, 0, -1):
            remote(zsend2.at[buf], zrecv2.at[buf, col], y_send.at[buf], y_recv.at[buf], (row, line(t))).start()
        zrecv2[buf, col] = total

    def env_end(buf):
        whole = zrecv2.at[buf, 0 : COLS - 1]
        remote(whole, whole, y_send.at[buf], y_recv.at[buf], (row, line(1))).wait_recv()
        total = zrecv2[buf, 0]
        for c in range(1, COLS):
            total = total + zrecv2[buf, c]
        return (slow_coupling * own_charge) * total

    def gather_start(g, pos):
        gath[g, row] = pos
        for t in range(ROWS - 1, 0, -1):
            remote(gath.at[g, row], gath.at[g, row], g_send.at[g], g_recv.at[g, row], (peer(t), col)).start()
        for comp in range(3):
            line_ = pos[comp : comp + 1, :]
            mat[comp, pl.ds(row, 1), :] = line_
            if comp < 2:
                line_ = line_ + corner[comp : comp + 1, :]
            for h in range(2):
                acol[comp, 128 * h : 128 * h + 128, :] = column(line_[:, 128 * h : 128 * h + 128])
        facc[...] = jnp.zeros_like(facc)

    def arrive(g, t):
        r = peer(t)
        slot = gath.at[g, r]
        remote(slot, slot, g_send.at[g], g_recv.at[g, r], (r, col)).wait_recv()
        for comp in range(3):
            mat[comp, pl.ds(r, 1), :] = gath[g, r, comp : comp + 1, :]

    def fast_row(g, t):
        r = peer(t)
        tile = gath[g, r]
        lines = (
            tile[0:1] + corner[0:1, :],
            tile[1:2] + corner[1:2, :],
            tile[2:3],
            charge_ref[pl.ds(r, 1), :],
        )
        halves = [[jnp.broadcast_to(v[:, 128 * h : 128 * h + 128], (8, 128)) for v in lines] for h in range(2)]
        for i in range(MOL // 8):
            x = acol[0, 8 * i : 8 * i + 8, :]
            y = acol[1, 8 * i : 8 * i + 8, :]
            z = acol[2, 8 * i : 8 * i + 8, :]
            fx = facc[0, 8 * i : 8 * i + 8, :]
            fy = facc[1, 8 * i : 8 * i + 8, :]
            fz = facc[2, 8 * i : 8 * i + 8, :]
            for ox, oy, oz, oq in halves:
                dx, dy, dz = x - ox, y - oy, z - oz
                s = (dx * dx + dy * dy) + (dz * dz + 1.0)
                inv = lax.rsqrt(s)
                w = (inv * inv) * (inv * oq)
                fx, fy, fz = fx + w * dx, fy + w * dy, fz + w * dz
            facc[0, 8 * i : 8 * i + 8, :] = fx
            facc[1, 8 * i : 8 * i + 8, :] = fy
            facc[2, 8 * i : 8 * i + 8, :] = fz

    def fast_rows(g, t0, t1, waiting):
        def body(t, carry):
            if waiting:
                arrive(g, t)
            fast_row(g, t)
            return carry

        lax.fori_loop(t0, t1, body, 0)

    def arrivals(g, t0, t1):
        def body(t, carry):
            arrive(g, t)
            return carry

        lax.fori_loop(t0, t1, body, 0)

    def fast_end(pos):
        d = [jnp.broadcast_to(pos[comp : comp + 1, :], (ROWS, MOL)) - mat[comp] for comp in range(3)]
        s = (d[0] * d[0] + d[1] * d[1]) + (d[2] * d[2] + 1.0)
        inv = lax.rsqrt(s)
        w = (inv * inv) * (inv * barred[...])
        out = []
        for comp in range(3):
            parts = [
                jnp.sum(jnp.transpose(facc[comp, 128 * h : 128 * h + 128, :]), axis=0, keepdims=True) for h in range(2)
            ]
            total = jnp.concatenate(parts, axis=1)
            out.append(total - jnp.sum(w * d[comp], axis=0, keepdims=True))
        out.append(jnp.zeros((1, MOL), jnp.float32))
        return (fast_coupling * own_charge) * jnp.concatenate(out, axis=0)

    loads[0].wait()
    loads[1].wait()
    fill_halo(0, spos_ref)
    loads[2].wait()
    loads[3].wait()
    wide = jnp.zeros((4, MOL - PIECE), jnp.float32)
    thin = jnp.zeros((1, PIECE), jnp.float32)
    for k, ref in enumerate((fpos_ref, fvel_ref)):
        value = jnp.concatenate([jnp.concatenate([ref[...], thin], axis=0), wide], axis=1)
        zown[4 * k : 4 * k + 4, :] = pltpu.roll(jnp.concatenate([value, value], axis=0), col * PIECE, 1)[0:4]
    pl.semaphore_wait(barrier, len(partners))
    for t in range(COLS - 1, 0, -1):
        remote(zown, zrecv.at[col], z_send, z_recv, (row, line(t))).start()
    for d in range(8):
        halo_copy(0, d).start()
    zrecv[col] = zown[...]
    for load in loads[4:]:
        load.wait()
    for h in range(2):
        charge_ref[:, 128 * h : 128 * h + 128] = charge_raw[pl.ds(h, ROWS, stride=2), :]
    own_charge = charge_ref[pl.ds(row, 1), :]
    owner = owner_line()
    corner[0:1, :] = lax.shift_right_logical(owner, 6).astype(jnp.float32)
    corner[1:2, :] = (owner & 63).astype(jnp.float32)
    index = lax.broadcasted_iota(jnp.int32, (ROWS, MOL), 0) * MOL + lax.broadcasted_iota(jnp.int32, (ROWS, MOL), 1)
    banned = excl_ref[...]
    hit = jnp.broadcast_to(banned[0:1, :], (ROWS, MOL)) == index
    for e in range(1, 4):
        hit = hit | (jnp.broadcast_to(banned[e : e + 1, :], (ROWS, MOL)) == index)
    barred[...] = jnp.where(hit, charge_ref[...], 0.0)
    fill_table(spos_ref)
    slow_start(spos_ref)

    whole = zrecv.at[0 : COLS - 1]
    remote(whole, whole, z_send, z_recv, (row, line(1))).wait_recv()
    both = zrecv[0]
    for c in range(1, COLS):
        both = both + zrecv[c]
    pos, vel = both[0:4], both[4:8]

    gather_start(0, pos)
    for d in range(8):
        halo_copy(0, d).wait_recv()
    slow_pairs(0, 0, 18)
    arrivals(0, 1, ROWS)
    env_rows(0)
    fast_rows(0, 0, ROWS, False)
    force = fast_end(pos)
    slow_pairs(0, 18, 22)
    env_middle(0)
    slow_pairs(0, 22, 32)
    slow_end()
    for comp in range(3):
        v = svel_ref[comp] + half_outer * ((slow_coupling * scharge_ref[...]) * sforce[comp])
        svel_out[comp] = v
        spos_out[comp] = spos_ref[comp] + outer_dt * v
    fill_halo(1, spos_out)
    for d in range(8):
        halo_copy(1, d).start()
    vel = vel + half_outer * env_end(0)
    for g in range(1, INNER + 1):
        vel = vel + (0.5 * inner_dt) * force
        pos = pos + inner_dt * vel
        gather_start(g, pos)
        if g == 1:
            fill_table(spos_out)
            slow_start(spos_out)
        elif g == 2:
            for d in range(8):
                halo_copy(1, d).wait_recv()
            slow_pairs(1, 0, 6)
        elif g == 3:
            slow_pairs(1, 6, 12)
        else:
            slow_pairs(1, 12, 18)
        fast_rows(g, 0, 1, False)
        if g < INNER:
            fast_rows(g, 1, ROWS, True)
            force = fast_end(pos)
            vel = vel + (0.5 * inner_dt) * force
        else:
            fast_rows(g, 1, 12, True)
            arrivals(g, 12, ROWS)
            env_direct()
            fast_rows(g, 12, ROWS, False)
            force = fast_end(pos)
            vel = vel + (0.5 * inner_dt) * force
    slow_pairs(1, 18, 32)
    slow_end()
    for comp in range(3):
        svel_out[comp] = svel_out[comp] + half_outer * ((slow_coupling * scharge_ref[...]) * sforce[comp])
    back = lax.rem(MOL - col * PIECE, MOL)

    def own_lanes(value):
        return pltpu.roll(jnp.concatenate([value, value], axis=0), back, 1)

    fpos_out[...] = own_lanes(pos)[0:3, 0:PIECE]
    vel = own_lanes(vel)
    scale = (half_outer * slow_coupling) * own_lanes(jnp.broadcast_to(own_charge, (4, MOL)))[0:1, 0:PIECE]
    total = env_total()
    for comp in range(3):
        part = pltpu.roll(jnp.broadcast_to(total, (8, 128)), 128 - 32 * comp, 1) if comp else total
        fvel_out[comp : comp + 1, :] = vel[comp : comp + 1, 0:PIECE] + scale * part[0:1, 0:PIECE]

    whole = zrecv.at[0 : COLS - 1]
    remote(whole, whole, z_send, z_recv, (row, line(1))).wait_send()
    for buf in range(2):
        for d in range(8):
            halo_copy(buf, d).wait_send()
    for ref, count, send, recv in (
        (erecv.at[0], ROWS, e_send.at[0], e_recv.at[0]),
        (zrecv2.at[0], COLS, y_send.at[0], y_recv.at[0]),
        (drecv, ROWS * COLS, d_send, d_recv),
    ):
        whole = ref.at[0 : count - 1]
        remote(whole, whole, send, recv, (row, line(1))).wait_send()
    for g in range(INNER + 1):
        whole = gath.at[g, 0 : ROWS - 1]
        remote(whole, whole, g_send.at[g], g_recv.at[g, 0], (row, line(1))).wait_send()


def finish(*refs):
    for a, b in zip(refs[:4], refs[4:]):
        b[...] = a[...]


def per_device(fast_pos, fast_vel, fast_charge, fast_owner, exclusions, slow_pos, slow_vel, slow_charge, neighbours):
    charge = fast_charge.reshape(FAST // 128, 128)
    owner = fast_owner.reshape(FAST // 128, 128)
    excl = exclusions.T
    f32 = jnp.float32
    vmem = pl.BlockSpec(memory_space=pltpu.VMEM)
    hbm = pl.BlockSpec(memory_space=pltpu.HBM)
    dma = pltpu.SemaphoreType.DMA
    outs = pl.pallas_call(
        kernel,
        out_shape=(
            jax.ShapeDtypeStruct((3, PIECE), f32),
            jax.ShapeDtypeStruct((3, PIECE), f32),
            jax.ShapeDtypeStruct((3, CELLS, CELL), f32),
            jax.ShapeDtypeStruct((3, CELLS, CELL), f32),
        ),
        in_specs=[hbm] * 9,
        out_specs=(vmem,) * 4,
        scratch_shapes=[
            pltpu.VMEM((3, PIECE), f32),
            pltpu.VMEM((3, PIECE), f32),
            pltpu.VMEM((FAST // 128, 128), f32),
            pltpu.VMEM((8, 128), jnp.int32),
            pltpu.VMEM((4, MOL), jnp.int32),
            pltpu.VMEM((3, CELLS, CELL), f32),
            pltpu.VMEM((3, CELLS, CELL), f32),
            pltpu.VMEM((CELLS, CELL), f32),
            pltpu.SMEM((NBR, CR, CC), jnp.int32),
            pltpu.VMEM((ROWS, MOL), f32),
            dma((9,)),
            pltpu.VMEM((COLS, 8, MOL), f32),
            pltpu.VMEM((INNER + 1, ROWS, 4, MOL), f32),
            pltpu.VMEM((3, ROWS, MOL), f32),
            pltpu.VMEM((2, ROWS, 4, MOL), f32),
            pltpu.VMEM((2, ROWS, 4, MOL), f32),
            pltpu.VMEM((2, 4, MOL), f32),
            pltpu.VMEM((2, COLS, 4, MOL), f32),
            pltpu.VMEM((3, MOL, 128), f32),
            pltpu.VMEM((3, MOL, 128), f32),
            pltpu.VMEM((CR + 4, CC + 4, 4, CELL), f32),
            pltpu.VMEM((CR + 4, CC + 4, 4, CELL), f32),
            pltpu.VMEM((3, CELL, CELL), f32),
            pltpu.VMEM((3, CELL, CELL), f32),
            pltpu.VMEM((3, CELL, CELL), f32),
            pltpu.VMEM((3, CELL, CELL), f32),
            pltpu.VMEM((3, CELLS, CELL), f32),
            pltpu.VMEM((4 * CELL, MOL), f32),
            pltpu.VMEM((8, MOL), f32),
            pltpu.VMEM((ROWS * COLS, 1, 128), f32),
            pltpu.VMEM((ROWS * COLS, 1, 128), f32),
            pltpu.VMEM((2, MOL), f32),
            pltpu.VMEM((ROWS, MOL), f32),
            dma,
            dma,
            dma((INNER + 1,)),
            dma((INNER + 1, ROWS)),
            dma((2,)),
            dma((2,)),
            dma((2,)),
            dma((2,)),
            dma((2, 8)),
            dma((2, 8)),
            dma,
            dma,
        ],
        compiler_params=pltpu.CompilerParams(
            collective_id=0, has_side_effects=True, vmem_limit_bytes=VMEM
        ),
    )(
        fast_pos,
        fast_vel,
        charge,
        owner,
        excl,
        slow_pos.reshape(3, CELLS, CELL),
        slow_vel.reshape(3, CELLS, CELL),
        slow_charge.reshape(CELLS, CELL),
        neighbours.transpose(2, 0, 1),
    )
    outs = pl.pallas_call(
        finish, out_shape=[jax.ShapeDtypeStruct(o.shape, f32) for o in outs], in_specs=[vmem] * 4, out_specs=[vmem] * 4,
        compiler_params=pltpu.CompilerParams(vmem_limit_bytes=VMEM),
    )(*outs)
    fpos, fvel, spos, svel = outs
    return fpos, fvel, spos.reshape(3, CR, CC, CELL), svel.reshape(3, CR, CC, CELL)


def solution(mesh):
    specs = (
        P(None, ("row", "col")),
        P(None, ("row", "col")),
        P(),
        P(),
        P(),
        P(None, "row", "col", None),
        P(None, "row", "col", None),
        P("row", "col", None),
        P("row", "col", None),
    )
    return jax.shard_map(
        per_device,
        mesh=mesh,
        in_specs=specs,
        out_specs=(specs[0], specs[1], specs[5], specs[6]),
        check_vma=False,
    )
```

```python
import jax
import jax.numpy as jnp
from jax import lax
from jax.experimental import pallas as pl
from jax.experimental.pallas import tpu as pltpu
from jax.sharding import PartitionSpec as P

MESH = pl.DeviceIdType.MESH
FAST = 4096
CELL = 128
NBR = 5
INNER = 4
ROWS, COLS = 16, 8
MOL = FAST // ROWS
PIECE = MOL // COLS
CR, CC = 4, 8
CELLS = CR * CC
VMEM = 67043328

ORDER = (0, 1, 3, 4, 12, 2, 8, 5, 7, 13, 15, 6, 14, 9, 11, 10)
LINE = 4
HOPS = (2, 1, 3, 0)

fast_coupling = 1.0
slow_coupling = 0.1
outer_dt = 0.2
half_outer = 0.5 * outer_dt
inner_dt = outer_dt / INNER

SIDES = [(a, b) for a in (-1, 0, 1) for b in (-1, 0, 1) if (a, b) != (0, 0)]


def column(row):
    return jnp.transpose(jnp.broadcast_to(row, (128, 128)))


def kernel(
    fpos_in, fvel_in, charge_in, owner_in, excl_in, spos_in, svel_in, scharge_in, nbr_in,
    fpos_out, fvel_out, spos_out, svel_out,
    fpos_ref, fvel_ref, charge_raw, owner_ref, excl_ref, spos_ref, svel_ref, scharge_ref, nbr_ref, charge_ref, in_sem,
    psend, precv, vsend, vrecv, gath, mat, esend, erecv, zsend2, zrecv2, acol, facc, halo_0, halo_1, scol_0, scol_1, sacc_0, sacc_1, sforce, table, dsend, drecv, corner, barred,
    p_send, p_recv, v_send, v_recv, g_send, g_recv, e_send, e_recv, y_send, y_recv, h_send, h_recv, d_send, d_recv,
):
    row = lax.axis_index("row")
    col = lax.axis_index("col")
    halos = (halo_0, halo_1)
    px, py, pz, pk = lax.div(row, 4), lax.rem(row, 4), lax.div(col, 2), lax.rem(col, 2)

    def peer(t):
        if isinstance(t, int):
            code = ORDER[t]
            dx, dy = code // 4, code % 4
        else:
            code = jnp.int32(0)
            for n in range(1, ROWS):
                code = jnp.where(t == n, ORDER[n], code)
            dx, dy = lax.div(code, 4), lax.rem(code, 4)
        return lax.rem(px + dx, 4) * 4 + lax.rem(py + dy, 4)

    def plane():
        for t in range(ROWS - 1, -1, -1):
            for k in (1 - pk, pk) if t else (1 - pk,):
                r = peer(t)
                yield (r, pz * 2 + k), r, k

    def line(t):
        return row, lax.rem(pz + t, LINE) * 2 + pk

    def everyone():
        for dx in HOPS:
            for dy in HOPS:
                for dz in HOPS:
                    for dk in (1, 0):
                        if dx or dy or dz or dk:
                            r = lax.rem(px + dx, 4) * 4 + lax.rem(py + dy, 4)
                            z, k = lax.rem(pz + dz, 4), lax.rem(pk + dk, 2)
                            yield (r, z * 2 + k), (k * 4 + z) * ROWS + r

    mine = (pk * 4 + pz) * ROWS + row

    def side(a, b):
        return lax.rem(row + (a + ROWS), ROWS), lax.rem(col + (b + COLS), COLS)

    def remote(src, dst, send, recv, to):
        return pltpu.make_async_remote_copy(
            src_ref=src, dst_ref=dst, send_sem=send, recv_sem=recv, device_id=to, device_id_type=MESH
        )

    loads = [
        pltpu.make_async_copy(src, dst, in_sem.at[k])
        for k, (src, dst) in enumerate(
            (
                (spos_in, spos_ref),
                (scharge_in, scharge_ref),
                (fpos_in, fpos_ref),
                (fvel_in, fvel_ref),
                (charge_in, charge_raw),
                (owner_in.at[0:8], owner_ref),
                (excl_in.at[:, pl.ds(pl.multiple_of(row * MOL, MOL), MOL)], excl_ref),
                (nbr_in, nbr_ref),
                (svel_in, svel_ref),
            )
        )
    ]
    for load in loads:
        load.start()

    barrier = pltpu.get_barrier_semaphore()
    for to, _ in everyone():
        pl.semaphore_signal(barrier, inc=1, device_id=to, device_id_type=MESH)

    def ordered(value):
        lane = lax.shift_right_logical(lax.broadcasted_iota(jnp.int32, (value.shape[0], 128), 1), 5)
        halves = []
        for k in range(2):
            out = None
            for z in range(4):
                c = 2 * z + k
                part = value[:, 128 * (c // 4) : 128 * (c // 4) + 128]
                shift = 32 * ((z - c) % 4)
                part = pltpu.roll(part, shift, 1) if shift else part
                out = part if out is None else jnp.where(lane == z, part, out)
            halves.append(out)
        return jnp.concatenate(halves, axis=1)

    def fill_halo(buf, pos):
        for r in range(CR):
            for comp in range(4):
                v = scharge_ref[r * CC : r * CC + CC, :] if comp == 3 else pos[comp, r * CC : r * CC + CC, :]
                for c in range(CC):
                    halos[buf][2 + r, 2 + c, comp : comp + 1, :] = v[c : c + 1, :]

    def halo_copy(buf, d):
        a, b = SIDES[d]
        rs, rd, rn = {-1: (2, 6, 2), 0: (2, 2, 4), 1: (4, 0, 2)}[a]
        cs, cd, cn = {-1: (2, 10, 2), 0: (2, 2, 8), 1: (8, 0, 2)}[b]
        return remote(
            halos[buf].at[rs : rs + rn, cs : cs + cn],
            halos[buf].at[rd : rd + rn, cd : cd + cn],
            h_send.at[buf, d],
            h_recv.at[buf, d],
            side(a, b),
        )

    scols, saccs = (scol_0, scol_1), (sacc_0, sacc_1)

    def slow_columns(pos, c, into):
        for comp in range(3):
            into[comp] = column(pos[comp, pl.ds(c, 1), :])

    def slow_sums(c, acc):
        for comp in range(3):
            sforce[comp, pl.ds(c, 1), :] = jnp.sum(jnp.transpose(acc[comp]), axis=0, keepdims=True)

    def slow_cell(halo, c, scol, sacc):
        r, k = lax.div(c, CC), lax.rem(c, CC)
        others = []
        for slot in range(NBR):
            o = nbr_ref[slot, r, k]
            dr = lax.div(o, 5)
            dc = o - 5 * dr
            tile = halo[r + dr, k + dc]
            others.append(
                (
                    jnp.broadcast_to(tile[0:1] + (dr - 2).astype(jnp.float32), (8, 128)),
                    jnp.broadcast_to(tile[1:2] + (dc - 2).astype(jnp.float32), (8, 128)),
                    jnp.broadcast_to(tile[2:3], (8, 128)),
                    jnp.broadcast_to(tile[3:4], (8, 128)),
                )
            )
        for i in range(16):
            x = scol[0, 8 * i : 8 * i + 8, :]
            y = scol[1, 8 * i : 8 * i + 8, :]
            z = scol[2, 8 * i : 8 * i + 8, :]
            fx = fy = fz = None
            for ox, oy, oz, oq in others:
                dx, dy, dz = x - ox, y - oy, z - oz
                s = (dx * dx + dy * dy) + (dz * dz + 0.5)
                inv = lax.rsqrt(s)
                w = (inv * inv) * (inv * oq)
                if fx is None:
                    fx, fy, fz = w * dx, w * dy, w * dz
                else:
                    fx, fy, fz = fx + w * dx, fy + w * dy, fz + w * dz
            sacc[0, 8 * i : 8 * i + 8, :] = fx
            sacc[1, 8 * i : 8 * i + 8, :] = fy
            sacc[2, 8 * i : 8 * i + 8, :] = fz

    def slow_start(pos):
        slow_columns(pos, 0, scol_0)
        sacc_1[...] = jnp.zeros_like(sacc_1)

    def slow_pairs(buf, c0, c1):
        pos = spos_out if buf else spos_ref

        def body(p, carry):
            c = 2 * p
            slow_cell(halos[buf], c, scol_0, sacc_0)
            slow_sums(lax.max(c - 1, 0), sacc_1)
            slow_columns(pos, c + 1, scol_1)
            slow_cell(halos[buf], c + 1, scol_1, sacc_1)
            slow_sums(c, sacc_0)
            slow_columns(pos, lax.min(c + 2, CELLS - 1), scol_0)
            return carry

        lax.fori_loop(c0 // 2, c1 // 2, body, 0)

    def slow_end():
        slow_sums(CELLS - 1, sacc_1)

    def owner_line():
        line_ = jnp.concatenate([owner_ref[0:1, :], owner_ref[1:2, :]], axis=1)
        return ordered(jnp.broadcast_to(line_, (8, MOL)))[0:1]

    def fill_table(pos):
        owner = owner_line()
        gr = lax.shift_right_logical(owner, 6) - row * CR
        gc = (owner & 63) - col * CC
        inside = (gr >= 0) & (gr < CR) & (gc >= 0) & (gc < CC)
        local = jnp.where(inside, gr * CC + gc, -1)
        ids = lax.broadcasted_iota(jnp.int32, (CELLS, MOL), 0)
        pick = jnp.where(jnp.broadcast_to(local, (CELLS, MOL)) == ids, 1.0, 0.0).astype(jnp.float32)
        for comp in range(4):
            data = scharge_ref[...] if comp == 3 else pos[comp]
            table[comp * CELL : (comp + 1) * CELL, :] = jnp.dot(
                jnp.transpose(data), pick, precision=lax.Precision.HIGHEST, preferred_element_type=jnp.float32
            )

    def env_partial():
        mx, my, mz = (jnp.concatenate([mat[comp, 0], mat[comp, 1]], axis=1) for comp in range(3))

        def body(jb, carry):
            fx, fy, fz = carry
            for k in range(4):
                j = jb * 4 + k
                ox, oy, oz, oq = (
                    jnp.broadcast_to(table[pl.ds(comp * CELL + j, 1), :], (ROWS, MOL)) for comp in range(4)
                )
                dx, dy, dz = mx - ox, my - oy, mz - oz
                s = (dx * dx + dy * dy) + (dz * dz + 0.5)
                inv = lax.rsqrt(s)
                w = (inv * inv) * (inv * oq)
                fx, fy, fz = fx + w * dx, fy + w * dy, fz + w * dz
            return fx, fy, fz

        zero = jnp.zeros((ROWS, MOL), jnp.float32)
        return lax.fori_loop(0, CELL // 4, body, (zero, zero, zero))

    def env_rows():
        force = env_partial()
        for r in range(ROWS):
            for k in range(2):
                for comp in range(3):
                    esend[r, k, comp : comp + 1, :] = force[comp][r : r + 1, 128 * k : 128 * k + 128]
                esend[r, k, 3:4, :] = jnp.zeros((1, 128), jnp.float32)
        for to, r, k in plane():
            remote(esend.at[r, k], erecv.at[row * 2 + pk], e_send, e_recv, to).start()
        erecv[row * 2 + pk] = esend[row, pk]

    def env_direct():
        force = env_partial()
        lane = lax.broadcasted_iota(jnp.int32, (ROWS, 128), 1)
        for c in range(COLS):
            h, j = c // 4, c % 4
            line_ = jnp.zeros((ROWS, 128), jnp.float32)
            for comp in range(3):
                part = force[comp][:, 128 * h : 128 * h + 128]
                shift = (32 * (comp - j)) % 128
                part = pltpu.roll(part, shift, 1) if shift else part
                line_ = jnp.where(lax.shift_right_logical(lane, 5) == comp, part, line_)
            for r in range(ROWS):
                dsend[c * ROWS + r] = line_[r : r + 1, :]
        for to, slot in everyone():
            remote(dsend.at[slot], drecv.at[mine], d_send, d_recv, to).start()
        drecv[mine] = dsend[mine]

    def env_total():
        whole = drecv.at[0 : ROWS * COLS - 1]
        remote(whole, whole, d_send, d_recv, line(1)).wait_recv()
        return jnp.sum(drecv[...], axis=0)

    def env_middle():
        whole = erecv.at[0 : 2 * ROWS - 1]
        remote(whole, whole, e_send, e_recv, line(1)).wait_recv()
        zsend2[...] = jnp.sum(erecv[...], axis=0)
        for t in (2, 1, 3):
            remote(zsend2, zrecv2.at[pz], y_send, y_recv, line(t)).start()
        zrecv2[pz] = zsend2[...]

    def env_end():
        whole = zrecv2.at[0 : LINE - 1]
        remote(whole, whole, y_send, y_recv, line(1)).wait_recv()
        return (slow_coupling * own_charge) * jnp.sum(zrecv2[...], axis=0)

    def gather_start(g, pos):
        gath[g, row, pk] = pos
        for to, r, k in plane():
            slot = gath.at[g, row, pk]
            remote(slot, slot, g_send.at[g], g_recv.at[g, row], to).start()
        for comp in range(3):
            mat[comp, pk, pl.ds(row, 1), :] = pos[comp : comp + 1, :]
        own_columns(pos)

    def own_columns(pos):
        for comp in range(3):
            line_ = pos[comp : comp + 1, :]
            if comp < 2:
                line_ = line_ + corner[comp, pk]
            acol[comp] = column(line_)
        facc[...] = jnp.zeros_like(facc)

    def arrive(g, t):
        r = peer(t)
        slot = gath.at[g, r]
        remote(slot, slot, g_send.at[g], g_recv.at[g, r], line(1)).wait_recv()
        for k in range(2):
            for comp in range(3):
                mat[comp, k, pl.ds(r, 1), :] = gath[g, r, k, comp : comp + 1, :]

    def arrive_core(g):
        slot = gath.at[g, row, 1 - pk]
        remote(slot, slot, g_send.at[g], g_recv.at[g, row], line(1)).wait_recv()
        for comp in range(3):
            mat[comp, 1 - pk, pl.ds(row, 1), :] = gath[g, row, 1 - pk, comp : comp + 1, :]

    def fast_row(g, t):
        r = peer(t)
        halves = [
            (
                mat[0, h, pl.ds(r, 1), :] + corner[0, h],
                mat[1, h, pl.ds(r, 1), :] + corner[1, h],
                mat[2, h, pl.ds(r, 1), :],
                charge_ref[h, pl.ds(r, 1), :],
            )
            for h in range(2)
        ]
        halves = [[jnp.broadcast_to(v, (8, 128)) for v in lines] for lines in halves]
        for i in range(16):
            x = acol[0, 8 * i : 8 * i + 8, :]
            y = acol[1, 8 * i : 8 * i + 8, :]
            z = acol[2, 8 * i : 8 * i + 8, :]
            fx = facc[0, 8 * i : 8 * i + 8, :]
            fy = facc[1, 8 * i : 8 * i + 8, :]
            fz = facc[2, 8 * i : 8 * i + 8, :]
            for ox, oy, oz, oq in halves:
                dx, dy, dz = x - ox, y - oy, z - oz
                s = (dx * dx + dy * dy) + (dz * dz + 1.0)
                inv = lax.rsqrt(s)
                w = (inv * inv) * (inv * oq)
                fx, fy, fz = fx + w * dx, fy + w * dy, fz + w * dz
            facc[0, 8 * i : 8 * i + 8, :] = fx
            facc[1, 8 * i : 8 * i + 8, :] = fy
            facc[2, 8 * i : 8 * i + 8, :] = fz

    def fast_rows(g, t0, t1, waiting):
        def body(t, carry):
            if waiting:
                arrive(g, t)
            fast_row(g, t)
            return carry

        lax.fori_loop(t0, t1, body, 0)

    def arrivals(g, t0, t1):
        def body(t, carry):
            arrive(g, t)
            return carry

        lax.fori_loop(t0, t1, body, 0)

    def fast_end(pos):
        d = [jnp.broadcast_to(pos[comp : comp + 1, :], (ROWS, 128)) - mat[comp, pk] for comp in range(3)]
        s = (d[0] * d[0] + d[1] * d[1]) + (d[2] * d[2] + 1.0)
        inv = lax.rsqrt(s)
        w = (inv * inv) * (inv * barred[...])
        out = []
        for comp in range(3):
            total = jnp.sum(jnp.transpose(facc[comp]), axis=0, keepdims=True)
            out.append(total - jnp.sum(w * d[comp], axis=0, keepdims=True))
        out.append(jnp.zeros((1, 128), jnp.float32))
        return (fast_coupling * own_charge) * jnp.concatenate(out, axis=0)

    def packed(ref):
        value = jnp.concatenate([ref[...], jnp.zeros((3, 128 - PIECE), jnp.float32)], axis=1)
        out = jnp.broadcast_to(value[0:1], (8, 128))
        for comp in (1, 2):
            out = out + pltpu.roll(jnp.broadcast_to(value[comp : comp + 1], (8, 128)), PIECE * comp, 1)
        return out[0:1]

    loads[2].wait()
    loads[3].wait()
    psend[...] = packed(fpos_ref)
    vsend[...] = packed(fvel_ref)
    precv[mine] = psend[...]
    vrecv[pz] = vsend[...]
    pl.semaphore_wait(barrier, ROWS * COLS - 1)
    for to, _ in everyone():
        remote(psend, precv.at[mine], p_send, p_recv, to).start()
    loads[0].wait()
    loads[1].wait()
    fill_halo(0, spos_ref)
    for d in range(8):
        halo_copy(0, d).start()
    for t in (2, 1, 3):
        remote(vsend, vrecv.at[pz], v_send, v_recv, line(t)).start()
    for load in loads[4:]:
        load.wait()
    raw = [charge_raw[pl.ds(h, ROWS, stride=2), :] for h in range(2)]
    charges = ordered(jnp.concatenate(raw, axis=1))
    for h in range(2):
        charge_ref[h] = charges[:, 128 * h : 128 * h + 128]
    own_charge = charge_ref[pk, pl.ds(row, 1), :]
    owner = owner_line()
    for h in range(2):
        corner[0, h] = lax.shift_right_logical(owner[:, 128 * h : 128 * h + 128], 6).astype(jnp.float32)
        corner[1, h] = (owner[:, 128 * h : 128 * h + 128] & 63).astype(jnp.float32)
    member = lax.broadcasted_iota(jnp.int32, (ROWS, 128), 0)
    other = 1 - pk
    banned = lax.shift_right_logical(ordered(jnp.concatenate([excl_ref[...], excl_ref[...]], axis=0)), 8)
    banned = banned[:, 0:128] * other + banned[:, 128:256] * pk
    hit = jnp.broadcast_to(banned[0:1, :], (ROWS, 128)) == member
    for e in range(1, 4):
        hit = hit | (jnp.broadcast_to(banned[e : e + 1, :], (ROWS, 128)) == member)
    barred[...] = jnp.where(hit, charge_ref[pk], 0.0)
    fill_table(spos_ref)
    slow_start(spos_ref)
    for d in range(8):
        halo_copy(0, d).wait_recv()
    slow_pairs(0, 0, 8)

    whole = precv.at[0 : ROWS * COLS - 1]
    remote(whole, whole, p_send, p_recv, line(1)).wait_recv()
    lane = lax.shift_right_logical(lax.broadcasted_iota(jnp.int32, (ROWS, 128), 1), 5)
    for k in range(2):
        blocks = [precv[(k * 4 + z) * ROWS : (k * 4 + z) * ROWS + ROWS, 0, :] for z in range(4)]
        for comp in range(3):
            out = None
            for z in range(4):
                shift = (32 * (z - comp)) % 128
                part = pltpu.roll(blocks[z], shift, 1) if shift else blocks[z]
                out = part if out is None else jnp.where(lane == z, part, out)
            mat[comp, k] = out
    env_rows()
    zero_line = jnp.zeros((1, 128), jnp.float32)
    pos = jnp.concatenate([mat[comp, pk, pl.ds(row, 1), :] for comp in range(3)] + [zero_line], axis=0)
    own_columns(pos)
    fast_rows(0, 0, ROWS, False)
    force = fast_end(pos)
    whole = vrecv.at[0 : LINE - 1]
    remote(whole, whole, v_send, v_recv, line(1)).wait_recv()
    rows = []
    lane = lax.shift_right_logical(lax.broadcasted_iota(jnp.int32, (8, 128), 1), 5)
    for comp in range(3):
        out = None
        for z in range(LINE):
            shift = (32 * (z - comp)) % 128
            part = jnp.broadcast_to(vrecv[z], (8, 128))
            part = pltpu.roll(part, shift, 1) if shift else part
            out = part if out is None else jnp.where(lane == z, part, out)
        rows.append(out[0:1])
    vel = jnp.concatenate(rows + [zero_line], axis=0)
    slow_pairs(0, 8, 18)
    env_middle()
    slow_pairs(0, 18, 28)
    vel = vel + half_outer * env_end()
    for g in range(1, INNER + 1):
        vel = vel + (0.5 * inner_dt) * force
        pos = pos + inner_dt * vel
        gather_start(g, pos)
        if g == 1:
            slow_pairs(0, 28, 32)
            slow_end()
            for comp in range(3):
                v = svel_ref[comp] + half_outer * ((slow_coupling * scharge_ref[...]) * sforce[comp])
                svel_out[comp] = v
                spos_out[comp] = spos_ref[comp] + outer_dt * v
            fill_halo(1, spos_out)
            for d in range(8):
                halo_copy(1, d).start()
            slow_start(spos_out)
        elif g == 2:
            for d in range(8):
                halo_copy(1, d).wait_recv()
            slow_pairs(1, 0, 10)
        elif g == 3:
            slow_pairs(1, 10, 20)
        else:
            fill_table(spos_out)
            slow_pairs(1, 20, 24)
        arrive_core(g)
        fast_rows(g, 0, 1, False)
        if g < INNER:
            fast_rows(g, 1, ROWS, True)
            force = fast_end(pos)
            vel = vel + (0.5 * inner_dt) * force
        else:
            fast_rows(g, 1, 12, True)
            arrivals(g, 12, ROWS)
            env_direct()
            fast_rows(g, 12, ROWS, False)
            force = fast_end(pos)
            vel = vel + (0.5 * inner_dt) * force
    slow_pairs(1, 24, 32)
    slow_end()
    for comp in range(3):
        svel_out[comp] = svel_out[comp] + half_outer * ((slow_coupling * scharge_ref[...]) * sforce[comp])
    back = lax.rem(128 - pz * PIECE, 128)

    def own_lanes(value):
        return pltpu.roll(jnp.concatenate([value, value], axis=0), back, 1)

    fpos_out[...] = own_lanes(pos)[0:3, 0:PIECE]
    vel = own_lanes(vel)
    scale = (half_outer * slow_coupling) * own_lanes(jnp.broadcast_to(own_charge, (4, 128)))[0:1, 0:PIECE]
    total = env_total()
    for comp in range(3):
        part = pltpu.roll(jnp.broadcast_to(total, (8, 128)), 128 - 32 * comp, 1) if comp else total
        fvel_out[comp : comp + 1, :] = vel[comp : comp + 1, 0:PIECE] + scale * part[0:1, 0:PIECE]

    for buf in range(2):
        for d in range(8):
            halo_copy(buf, d).wait_send()
    sent = [
        (precv, ROWS * COLS, p_send, p_recv),
        (vrecv, LINE, v_send, v_recv),
        (erecv, 2 * ROWS, e_send, e_recv),
        (zrecv2, LINE, y_send, y_recv),
        (drecv, ROWS * COLS, d_send, d_recv),
    ]
    for ref, count, send, recv in sent:
        whole = ref.at[0 : count - 1]
        remote(whole, whole, send, recv, line(1)).wait_send()
    for g in range(1, INNER + 1):
        whole = erecv.at[0 : 2 * ROWS - 1]
        remote(whole, whole, g_send.at[g], g_recv.at[g, 0], line(1)).wait_send()


def finish(*refs):
    for a, b in zip(refs[:4], refs[4:]):
        b[...] = a[...]


def per_device(fast_pos, fast_vel, fast_charge, fast_owner, exclusions, slow_pos, slow_vel, slow_charge, neighbours):
    charge = fast_charge.reshape(FAST // 128, 128)
    owner = fast_owner.reshape(FAST // 128, 128)
    excl = exclusions.T
    f32 = jnp.float32
    vmem = pl.BlockSpec(memory_space=pltpu.VMEM)
    hbm = pl.BlockSpec(memory_space=pltpu.HBM)
    dma = pltpu.SemaphoreType.DMA
    outs = pl.pallas_call(
        kernel,
        out_shape=(
            jax.ShapeDtypeStruct((3, PIECE), f32),
            jax.ShapeDtypeStruct((3, PIECE), f32),
            jax.ShapeDtypeStruct((3, CELLS, CELL), f32),
            jax.ShapeDtypeStruct((3, CELLS, CELL), f32),
        ),
        in_specs=[hbm] * 9,
        out_specs=(vmem,) * 4,
        scratch_shapes=[
            pltpu.VMEM((3, PIECE), f32),
            pltpu.VMEM((3, PIECE), f32),
            pltpu.VMEM((FAST // 128, 128), f32),
            pltpu.VMEM((8, 128), jnp.int32),
            pltpu.VMEM((4, MOL), jnp.int32),
            pltpu.VMEM((3, CELLS, CELL), f32),
            pltpu.VMEM((3, CELLS, CELL), f32),
            pltpu.VMEM((CELLS, CELL), f32),
            pltpu.SMEM((NBR, CR, CC), jnp.int32),
            pltpu.VMEM((2, ROWS, 128), f32),
            dma((9,)),
            pltpu.VMEM((1, 128), f32),
            pltpu.VMEM((ROWS * COLS, 1, 128), f32),
            pltpu.VMEM((1, 128), f32),
            pltpu.VMEM((LINE, 1, 128), f32),
            pltpu.VMEM((INNER + 1, ROWS, 2, 4, 128), f32),
            pltpu.VMEM((3, 2, ROWS, 128), f32),
            pltpu.VMEM((ROWS, 2, 4, 128), f32),
            pltpu.VMEM((2 * ROWS, 4, 128), f32),
            pltpu.VMEM((4, 128), f32),
            pltpu.VMEM((LINE, 4, 128), f32),
            pltpu.VMEM((3, 128, 128), f32),
            pltpu.VMEM((3, 128, 128), f32),
            pltpu.VMEM((CR + 4, CC + 4, 4, CELL), f32),
            pltpu.VMEM((CR + 4, CC + 4, 4, CELL), f32),
            pltpu.VMEM((3, CELL, CELL), f32),
            pltpu.VMEM((3, CELL, CELL), f32),
            pltpu.VMEM((3, CELL, CELL), f32),
            pltpu.VMEM((3, CELL, CELL), f32),
            pltpu.VMEM((3, CELLS, CELL), f32),
            pltpu.VMEM((4 * CELL, MOL), f32),
            pltpu.VMEM((ROWS * COLS, 1, 128), f32),
            pltpu.VMEM((ROWS * COLS, 1, 128), f32),
            pltpu.VMEM((2, 2, 1, 128), f32),
            pltpu.VMEM((ROWS, 128), f32),
            dma,
            dma,
            dma,
            dma,
            dma((INNER + 1,)),
            dma((INNER + 1, ROWS)),
            dma,
            dma,
            dma,
            dma,
            dma((2, 8)),
            dma((2, 8)),
            dma,
            dma,
        ],
        compiler_params=pltpu.CompilerParams(
            collective_id=0, has_side_effects=True, vmem_limit_bytes=VMEM
        ),
    )(
        fast_pos,
        fast_vel,
        charge,
        owner,
        excl,
        slow_pos.reshape(3, CELLS, CELL),
        slow_vel.reshape(3, CELLS, CELL),
        slow_charge.reshape(CELLS, CELL),
        neighbours.transpose(2, 0, 1),
    )
    outs = pl.pallas_call(
        finish, out_shape=[jax.ShapeDtypeStruct(o.shape, f32) for o in outs], in_specs=[vmem] * 4, out_specs=[vmem] * 4,
        compiler_params=pltpu.CompilerParams(vmem_limit_bytes=VMEM),
    )(*outs)
    fpos, fvel, spos, svel = outs
    return fpos, fvel, spos.reshape(3, CR, CC, CELL), svel.reshape(3, CR, CC, CELL)


def solution(mesh):
    specs = (
        P(None, ("row", "col")),
        P(None, ("row", "col")),
        P(),
        P(),
        P(),
        P(None, "row", "col", None),
        P(None, "row", "col", None),
        P("row", "col", None),
        P("row", "col", None),
    )
    return jax.shard_map(
        per_device,
        mesh=mesh,
        in_specs=specs,
        out_specs=(specs[0], specs[1], specs[5], specs[6]),
        check_vma=False,
    )
```

```python
import jax
import jax.numpy as jnp
from jax import lax
from jax.experimental import pallas as pl
from jax.experimental.pallas import tpu as pltpu
from jax.sharding import PartitionSpec as P

MESH = pl.DeviceIdType.MESH
FAST = 4096
CELL = 128
NBR = 5
INNER = 4
ROWS, COLS = 16, 8
MOL = FAST // ROWS
PIECE = MOL // COLS
CR, CC = 4, 8
CELLS = CR * CC
VMEM = 67043328

ORDER = (0, 1, 3, 4, 12, 2, 8, 5, 7, 13, 15, 6, 14, 9, 11, 10)
LINE = 4
HOPS = (2, 1, 3, 0)

fast_coupling = 1.0
slow_coupling = 0.1
outer_dt = 0.2
half_outer = 0.5 * outer_dt
inner_dt = outer_dt / INNER

SIDES = [(a, b) for a in (-1, 0, 1) for b in (-1, 0, 1) if (a, b) != (0, 0)]


def column(row):
    return jnp.transpose(jnp.broadcast_to(row, (128, 128)))


def kernel(
    fpos_in, fvel_in, charge_in, owner_in, excl_in, spos_in, svel_in, scharge_in, nbr_in,
    fpos_out, fvel_out, spos_out, svel_out,
    fpos_ref, fvel_ref, charge_raw, owner_ref, excl_ref, spos_ref, svel_ref, scharge_ref, nbr_ref, charge_ref, in_sem,
    psend, precv, vsend, vrecv, gath, mat, esend, erecv, zsend2, zrecv2, acol, facc, halo_0, halo_1, scol_0, scol_1, sacc_0, sacc_1, sforce, table, eforce, dsend, drecv, corner, barred,
    p_send, p_recv, v_send, v_recv, g_send, g_recv, e_send, e_recv, y_send, y_recv, h_send, h_recv, d_send, d_recv,
):
    row = lax.axis_index("row")
    col = lax.axis_index("col")
    halos = (halo_0, halo_1)
    px, py, pz, pk = lax.div(row, 4), lax.rem(row, 4), lax.div(col, 2), lax.rem(col, 2)

    near = lax.div(px, 2)

    def peer(t):
        if isinstance(t, int):
            code = ORDER[t]
            dx, dy = code // 4, code % 4
        else:
            code = jnp.int32(0)
            for n in range(1, ROWS):
                code = jnp.where(t == n, ORDER[n], code)
            dx, dy = lax.div(code, 4), lax.rem(code, 4)
        return lax.rem(px + dx, 4) * 4 + lax.rem(py + dy, 4)

    def plane():
        for t in range(ROWS - 1, -1, -1):
            for k in (1 - pk, pk) if t else (1 - pk,):
                r = peer(t)
                yield (r, pz * 2 + k), r, k

    def line(t):
        return row, lax.rem(pz + t, LINE) * 2 + pk

    def everyone():
        for dx in HOPS:
            for dy in HOPS:
                for dz in HOPS:
                    for dk in (1, 0):
                        if dx or dy or dz or dk:
                            r = lax.rem(px + dx, 4) * 4 + lax.rem(py + dy, 4)
                            z, k = lax.rem(pz + dz, 4), lax.rem(pk + dk, 2)
                            yield (r, z * 2 + k), (k * 4 + z) * ROWS + r

    mine = (pk * 4 + pz) * ROWS + row

    def side(a, b):
        return lax.rem(row + (a + ROWS), ROWS), lax.rem(col + (b + COLS), COLS)

    def remote(src, dst, send, recv, to):
        return pltpu.make_async_remote_copy(
            src_ref=src, dst_ref=dst, send_sem=send, recv_sem=recv, device_id=to, device_id_type=MESH
        )

    loads = [
        pltpu.make_async_copy(src, dst, in_sem.at[k])
        for k, (src, dst) in enumerate(
            (
                (spos_in, spos_ref),
                (scharge_in, scharge_ref),
                (fpos_in, fpos_ref),
                (fvel_in, fvel_ref),
                (charge_in, charge_raw),
                (owner_in.at[0:8], owner_ref),
                (excl_in.at[:, pl.ds(pl.multiple_of(row * MOL, MOL), MOL)], excl_ref),
                (nbr_in, nbr_ref),
                (svel_in, svel_ref),
            )
        )
    ]
    for load in loads:
        load.start()

    barrier = pltpu.get_barrier_semaphore()
    for to, _ in everyone():
        pl.semaphore_signal(barrier, inc=1, device_id=to, device_id_type=MESH)

    def ordered(value):
        lane = lax.shift_right_logical(lax.broadcasted_iota(jnp.int32, (value.shape[0], 128), 1), 5)
        halves = []
        for k in range(2):
            out = None
            for z in range(4):
                c = 2 * z + k
                part = value[:, 128 * (c // 4) : 128 * (c // 4) + 128]
                shift = 32 * ((z - c) % 4)
                part = pltpu.roll(part, shift, 1) if shift else part
                out = part if out is None else jnp.where(lane == z, part, out)
            halves.append(out)
        return jnp.concatenate(halves, axis=1)

    def fill_halo(buf, pos):
        for r in range(CR):
            for comp in range(4):
                v = scharge_ref[r * CC : r * CC + CC, :] if comp == 3 else pos[comp, r * CC : r * CC + CC, :]
                for c in range(CC):
                    halos[buf][2 + r, 2 + c, comp : comp + 1, :] = v[c : c + 1, :]

    def halo_copy(buf, d):
        a, b = SIDES[d]
        rs, rd, rn = {-1: (2, 6, 2), 0: (2, 2, 4), 1: (4, 0, 2)}[a]
        cs, cd, cn = {-1: (2, 10, 2), 0: (2, 2, 8), 1: (8, 0, 2)}[b]
        return remote(
            halos[buf].at[rs : rs + rn, cs : cs + cn],
            halos[buf].at[rd : rd + rn, cd : cd + cn],
            h_send.at[buf, d],
            h_recv.at[buf, d],
            side(a, b),
        )

    scols, saccs = (scol_0, scol_1), (sacc_0, sacc_1)

    def slow_columns(pos, c, into):
        for comp in range(3):
            into[comp] = column(pos[comp, pl.ds(c, 1), :])

    def slow_sums(c, acc):
        for comp in range(3):
            sforce[comp, pl.ds(c, 1), :] = jnp.sum(jnp.transpose(acc[comp]), axis=0, keepdims=True)

    def slow_cell(halo, c, scol, sacc):
        r, k = lax.div(c, CC), lax.rem(c, CC)
        others = []
        for slot in range(NBR):
            o = nbr_ref[slot, r, k]
            dr = lax.div(o, 5)
            dc = o - 5 * dr
            tile = halo[r + dr, k + dc]
            others.append(
                (
                    jnp.broadcast_to(tile[0:1] + (dr - 2).astype(jnp.float32), (8, 128)),
                    jnp.broadcast_to(tile[1:2] + (dc - 2).astype(jnp.float32), (8, 128)),
                    jnp.broadcast_to(tile[2:3], (8, 128)),
                    jnp.broadcast_to(tile[3:4], (8, 128)),
                )
            )
        for i in range(16):
            x = scol[0, 8 * i : 8 * i + 8, :]
            y = scol[1, 8 * i : 8 * i + 8, :]
            z = scol[2, 8 * i : 8 * i + 8, :]
            fx = fy = fz = None
            for ox, oy, oz, oq in others:
                dx, dy, dz = x - ox, y - oy, z - oz
                s = (dx * dx + dy * dy) + (dz * dz + 0.5)
                inv = lax.rsqrt(s)
                w = (inv * inv) * (inv * oq)
                if fx is None:
                    fx, fy, fz = w * dx, w * dy, w * dz
                else:
                    fx, fy, fz = fx + w * dx, fy + w * dy, fz + w * dz
            sacc[0, 8 * i : 8 * i + 8, :] = fx
            sacc[1, 8 * i : 8 * i + 8, :] = fy
            sacc[2, 8 * i : 8 * i + 8, :] = fz

    def slow_start(pos):
        slow_columns(pos, 0, scol_0)
        sacc_1[...] = jnp.zeros_like(sacc_1)

    def slow_pairs(buf, c0, c1):
        pos = spos_out if buf else spos_ref

        def body(p, carry):
            c = 2 * p
            slow_cell(halos[buf], c, scol_0, sacc_0)
            slow_sums(lax.max(c - 1, 0), sacc_1)
            slow_columns(pos, c + 1, scol_1)
            slow_cell(halos[buf], c + 1, scol_1, sacc_1)
            slow_sums(c, sacc_0)
            slow_columns(pos, lax.min(c + 2, CELLS - 1), scol_0)
            return carry

        lax.fori_loop(c0 // 2, c1 // 2, body, 0)

    def slow_end():
        slow_sums(CELLS - 1, sacc_1)

    def owner_line():
        line_ = jnp.concatenate([owner_ref[0:1, :], owner_ref[1:2, :]], axis=1)
        return ordered(jnp.broadcast_to(line_, (8, MOL)))[0:1]

    def fill_table(pos):
        owner = owner_line()
        gr = lax.shift_right_logical(owner, 6) - row * CR
        gc = (owner & 63) - col * CC
        inside = (gr >= 0) & (gr < CR) & (gc >= 0) & (gc < CC)
        local = jnp.where(inside, gr * CC + gc, -1)
        ids = lax.broadcasted_iota(jnp.int32, (CELLS, MOL), 0)
        pick = jnp.where(jnp.broadcast_to(local, (CELLS, MOL)) == ids, 1.0, 0.0).astype(jnp.float32)
        for comp in range(4):
            data = scharge_ref[...] if comp == 3 else pos[comp]
            table[comp * CELL : (comp + 1) * CELL, :] = jnp.dot(
                jnp.transpose(data), pick, precision=lax.Precision.HIGHEST, preferred_element_type=jnp.float32
            )

    def env_half(part):
        rows8 = pl.ds(pl.multiple_of(part * 8, 8), 8)
        mx, my, mz = (jnp.concatenate([mat[comp, h, rows8, :] for h in range(2)], axis=1) for comp in range(3))

        def body(jb, carry):
            fx, fy, fz = carry
            for n in range(8):
                j = jb * 8 + n
                ox, oy, oz, oq = (
                    jnp.broadcast_to(table[pl.ds(comp * CELL + j, 1), :], (8, MOL)) for comp in range(4)
                )
                dx, dy, dz = mx - ox, my - oy, mz - oz
                s = (dx * dx + dy * dy) + (dz * dz + 0.5)
                inv = lax.rsqrt(s)
                w = (inv * inv) * (inv * oq)
                fx, fy, fz = fx + w * dx, fy + w * dy, fz + w * dz
            return fx, fy, fz

        zero = jnp.zeros((8, MOL), jnp.float32)
        force = lax.fori_loop(0, CELL // 8, body, (zero, zero, zero))
        for comp in range(3):
            eforce[comp, rows8, :] = force[comp]

    def env_rows():
        for r in range(ROWS):
            for k in range(2):
                for comp in range(3):
                    esend[r, k, comp : comp + 1, :] = eforce[comp, r : r + 1, 128 * k : 128 * k + 128]
                esend[r, k, 3:4, :] = jnp.zeros((1, 128), jnp.float32)
        for to, r, k in plane():
            remote(esend.at[r, k], erecv.at[row * 2 + pk], e_send, e_recv, to).start()
        erecv[row * 2 + pk] = esend[row, pk]

    def env_direct():
        lane = lax.broadcasted_iota(jnp.int32, (ROWS, 128), 1)
        for c in range(COLS):
            h, j = c // 4, c % 4
            line_ = jnp.zeros((ROWS, 128), jnp.float32)
            for comp in range(3):
                part = eforce[comp, :, 128 * h : 128 * h + 128]
                shift = (32 * (comp - j)) % 128
                part = pltpu.roll(part, shift, 1) if shift else part
                line_ = jnp.where(lax.shift_right_logical(lane, 5) == comp, part, line_)
            for r in range(ROWS):
                dsend[c * ROWS + r] = line_[r : r + 1, :]
        for to, slot in everyone():
            remote(dsend.at[slot], drecv.at[mine], d_send, d_recv, to).start()
        drecv[mine] = dsend[mine]

    def env_total():
        whole = drecv.at[0 : ROWS * COLS - 1]
        remote(whole, whole, d_send, d_recv, line(1)).wait_recv()
        return jnp.sum(drecv[...], axis=0)

    def env_middle():
        whole = erecv.at[0 : 2 * ROWS - 1]
        remote(whole, whole, e_send, e_recv, line(1)).wait_recv()
        zsend2[...] = jnp.sum(erecv[...], axis=0)
        for t in (2, 1, 3):
            remote(zsend2, zrecv2.at[pz], y_send, y_recv, line(t)).start()
        zrecv2[pz] = zsend2[...]

    def env_end():
        whole = zrecv2.at[0 : LINE - 1]
        remote(whole, whole, y_send, y_recv, line(1)).wait_recv()
        return (slow_coupling * own_charge) * jnp.sum(zrecv2[...], axis=0)

    def gather_start(g, pos):
        gath[g, row, pk] = pos
        for to, r, k in plane():
            slot = gath.at[g, row, pk]
            remote(slot, slot, g_send.at[g], g_recv.at[g, row], to).start()
        for comp in range(3):
            mat[comp, pk, pl.ds(row, 1), :] = pos[comp : comp + 1, :]
        own_columns(pos)

    def own_columns(pos):
        for comp in range(3):
            line_ = pos[comp : comp + 1, :]
            if comp < 2:
                line_ = line_ + corner[comp, pk]
            acol[comp] = column(line_)
        facc[...] = jnp.zeros_like(facc)

    def arrive(g, r):
        slot = gath.at[g, r]
        remote(slot, slot, g_send.at[g], g_recv.at[g, r], line(1)).wait_recv()
        for k in range(2):
            for comp in range(3):
                mat[comp, k, pl.ds(r, 1), :] = gath[g, r, k, comp : comp + 1, :]

    def arrive_core(g):
        slot = gath.at[g, row, 1 - pk]
        remote(slot, slot, g_send.at[g], g_recv.at[g, row], line(1)).wait_recv()
        for comp in range(3):
            mat[comp, 1 - pk, pl.ds(row, 1), :] = gath[g, row, 1 - pk, comp : comp + 1, :]

    def fast_row(r):
        halves = [
            (
                mat[0, h, pl.ds(r, 1), :] + corner[0, h],
                mat[1, h, pl.ds(r, 1), :] + corner[1, h],
                mat[2, h, pl.ds(r, 1), :],
                charge_ref[h, pl.ds(r, 1), :],
            )
            for h in range(2)
        ]
        halves = [[jnp.broadcast_to(v, (8, 128)) for v in lines] for lines in halves]
        for i in range(16):
            x = acol[0, 8 * i : 8 * i + 8, :]
            y = acol[1, 8 * i : 8 * i + 8, :]
            z = acol[2, 8 * i : 8 * i + 8, :]
            fx = facc[0, 8 * i : 8 * i + 8, :]
            fy = facc[1, 8 * i : 8 * i + 8, :]
            fz = facc[2, 8 * i : 8 * i + 8, :]
            for ox, oy, oz, oq in halves:
                dx, dy, dz = x - ox, y - oy, z - oz
                s = (dx * dx + dy * dy) + (dz * dz + 1.0)
                inv = lax.rsqrt(s)
                w = (inv * inv) * (inv * oq)
                fx, fy, fz = fx + w * dx, fy + w * dy, fz + w * dz
            facc[0, 8 * i : 8 * i + 8, :] = fx
            facc[1, 8 * i : 8 * i + 8, :] = fy
            facc[2, 8 * i : 8 * i + 8, :] = fz

    def fast_rows(g, count, which, waiting=True, computing=True):
        def body(t, carry):
            r = which(t)
            if waiting:
                arrive(g, r)
            if computing:
                fast_row(r)
            return carry

        lax.fori_loop(0, count, body, 0)

    def same_x(t):
        return px * 4 + lax.rem(py + 1 + t, 4)

    def next_x(t):
        return (px + 1 - 2 * lax.rem(px, 2)) * 4 + lax.rem(py + t, 4)

    def far_x(t):
        return (1 - near) * 8 + t

    def fast_end(pos):
        d = [jnp.broadcast_to(pos[comp : comp + 1, :], (ROWS, 128)) - mat[comp, pk] for comp in range(3)]
        s = (d[0] * d[0] + d[1] * d[1]) + (d[2] * d[2] + 1.0)
        inv = lax.rsqrt(s)
        w = (inv * inv) * (inv * barred[...])
        out = []
        for comp in range(3):
            total = jnp.sum(jnp.transpose(facc[comp]), axis=0, keepdims=True)
            out.append(total - jnp.sum(w * d[comp], axis=0, keepdims=True))
        out.append(jnp.zeros((1, 128), jnp.float32))
        return (fast_coupling * own_charge) * jnp.concatenate(out, axis=0)

    def packed(ref):
        value = jnp.concatenate([ref[...], jnp.zeros((3, 128 - PIECE), jnp.float32)], axis=1)
        out = jnp.broadcast_to(value[0:1], (8, 128))
        for comp in (1, 2):
            out = out + pltpu.roll(jnp.broadcast_to(value[comp : comp + 1], (8, 128)), PIECE * comp, 1)
        return out[0:1]

    loads[2].wait()
    loads[3].wait()
    psend[...] = packed(fpos_ref)
    vsend[...] = packed(fvel_ref)
    precv[mine] = psend[...]
    vrecv[pz] = vsend[...]
    pl.semaphore_wait(barrier, ROWS * COLS - 1)
    for to, _ in everyone():
        remote(psend, precv.at[mine], p_send, p_recv.at[near], to).start()
    loads[0].wait()
    loads[1].wait()
    fill_halo(0, spos_ref)
    for d in range(8):
        halo_copy(0, d).start()
    for t in (2, 1, 3):
        remote(vsend, vrecv.at[pz], v_send, v_recv, line(t)).start()
    for load in loads[4:]:
        load.wait()
    raw = [charge_raw[pl.ds(h, ROWS, stride=2), :] for h in range(2)]
    charges = ordered(jnp.concatenate(raw, axis=1))
    for h in range(2):
        charge_ref[h] = charges[:, 128 * h : 128 * h + 128]
    own_charge = charge_ref[pk, pl.ds(row, 1), :]
    owner = owner_line()
    for h in range(2):
        corner[0, h] = lax.shift_right_logical(owner[:, 128 * h : 128 * h + 128], 6).astype(jnp.float32)
        corner[1, h] = (owner[:, 128 * h : 128 * h + 128] & 63).astype(jnp.float32)
    member = lax.broadcasted_iota(jnp.int32, (ROWS, 128), 0)
    other = 1 - pk
    banned = lax.shift_right_logical(ordered(jnp.concatenate([excl_ref[...], excl_ref[...]], axis=0)), 8)
    banned = banned[:, 0:128] * other + banned[:, 128:256] * pk
    hit = jnp.broadcast_to(banned[0:1, :], (ROWS, 128)) == member
    for e in range(1, 4):
        hit = hit | (jnp.broadcast_to(banned[e : e + 1, :], (ROWS, 128)) == member)
    barred[...] = jnp.where(hit, charge_ref[pk], 0.0)
    fill_table(spos_ref)
    slow_start(spos_ref)

    lane = lax.shift_right_logical(lax.broadcasted_iota(jnp.int32, (8, 128), 1), 5)
    for part in (near, 1 - near):
        whole = precv.at[0 : 63 if part is near else 64]
        remote(whole, whole, p_send, p_recv.at[part], line(1)).wait_recv()
        for k in range(2):
            blocks = [precv[pl.ds((k * 4 + z) * ROWS + part * 8, 8), 0, :] for z in range(4)]
            for comp in range(3):
                out = None
                for z in range(4):
                    shift = (32 * (z - comp)) % 128
                    block = pltpu.roll(blocks[z], shift, 1) if shift else blocks[z]
                    out = block if out is None else jnp.where(lane == z, block, out)
                mat[comp, k, pl.ds(pl.multiple_of(part * 8, 8), 8), :] = out
        env_half(part)
    env_rows()
    zero_line = jnp.zeros((1, 128), jnp.float32)
    pos = jnp.concatenate([mat[comp, pk, pl.ds(row, 1), :] for comp in range(3)] + [zero_line], axis=0)
    own_columns(pos)
    fast_rows(0, ROWS, lambda t: t, waiting=False)
    force = fast_end(pos)
    whole = vrecv.at[0 : LINE - 1]
    remote(whole, whole, v_send, v_recv, line(1)).wait_recv()
    rows = []
    lane = lax.shift_right_logical(lax.broadcasted_iota(jnp.int32, (8, 128), 1), 5)
    for comp in range(3):
        out = None
        for z in range(LINE):
            shift = (32 * (z - comp)) % 128
            part = jnp.broadcast_to(vrecv[z], (8, 128))
            part = pltpu.roll(part, shift, 1) if shift else part
            out = part if out is None else jnp.where(lane == z, part, out)
        rows.append(out[0:1])
    vel = jnp.concatenate(rows + [zero_line], axis=0)
    for d in range(8):
        halo_copy(0, d).wait_recv()
    slow_pairs(0, 0, 8)
    env_middle()
    slow_pairs(0, 8, 18)
    vel = vel + half_outer * env_end()
    for g in range(1, INNER + 1):
        vel = vel + (0.5 * inner_dt) * force
        pos = pos + inner_dt * vel
        gather_start(g, pos)
        if g == 1:
            slow_pairs(0, 18, 26)
        elif g == 2:
            slow_pairs(0, 26, 32)
            slow_end()
            for comp in range(3):
                v = svel_ref[comp] + half_outer * ((slow_coupling * scharge_ref[...]) * sforce[comp])
                svel_out[comp] = v
                spos_out[comp] = spos_ref[comp] + outer_dt * v
            fill_halo(1, spos_out)
            for d in range(8):
                halo_copy(1, d).start()
            slow_start(spos_out)
        elif g == 3:
            arrive_core(g)
            fast_row(row)
            for d in range(8):
                halo_copy(1, d).wait_recv()
            slow_pairs(1, 0, 8)
        else:
            fill_table(spos_out)
            slow_pairs(1, 8, 14)
        if g != 3:
            arrive_core(g)
            fast_row(row)
        if g < INNER:
            fast_rows(g, ROWS - 1, lambda t: peer(t + 1))
        else:
            fast_rows(g, 3, same_x)
            fast_rows(g, 2, next_x)
            fast_rows(g, 2, lambda t: next_x(t + 2), computing=False)
            env_half(near)
            fast_rows(g, 8, far_x, computing=False)
            env_half(1 - near)
            env_direct()
            fast_rows(g, 2, lambda t: next_x(t + 2), waiting=False)
            fast_rows(g, 8, far_x, waiting=False)
        force = fast_end(pos)
        vel = vel + (0.5 * inner_dt) * force
    slow_pairs(1, 14, 32)
    slow_end()
    for comp in range(3):
        svel_out[comp] = svel_out[comp] + half_outer * ((slow_coupling * scharge_ref[...]) * sforce[comp])
    back = lax.rem(128 - pz * PIECE, 128)

    def own_lanes(value):
        return pltpu.roll(jnp.concatenate([value, value], axis=0), back, 1)

    fpos_out[...] = own_lanes(pos)[0:3, 0:PIECE]
    vel = own_lanes(vel)
    scale = (half_outer * slow_coupling) * own_lanes(jnp.broadcast_to(own_charge, (4, 128)))[0:1, 0:PIECE]
    total = env_total()
    for comp in range(3):
        part = pltpu.roll(jnp.broadcast_to(total, (8, 128)), 128 - 32 * comp, 1) if comp else total
        fvel_out[comp : comp + 1, :] = vel[comp : comp + 1, 0:PIECE] + scale * part[0:1, 0:PIECE]

    for buf in range(2):
        for d in range(8):
            halo_copy(buf, d).wait_send()
    sent = [
        (precv, ROWS * COLS, p_send, p_recv.at[0]),
        (vrecv, LINE, v_send, v_recv),
        (erecv, 2 * ROWS, e_send, e_recv),
        (zrecv2, LINE, y_send, y_recv),
        (drecv, ROWS * COLS, d_send, d_recv),
    ]
    for ref, count, send, recv in sent:
        whole = ref.at[0 : count - 1]
        remote(whole, whole, send, recv, line(1)).wait_send()
    for g in range(1, INNER + 1):
        whole = erecv.at[0 : 2 * ROWS - 1]
        remote(whole, whole, g_send.at[g], g_recv.at[g, 0], line(1)).wait_send()


def finish(*refs):
    for a, b in zip(refs[:4], refs[4:]):
        b[...] = a[...]


def per_device(fast_pos, fast_vel, fast_charge, fast_owner, exclusions, slow_pos, slow_vel, slow_charge, neighbours):
    charge = fast_charge.reshape(FAST // 128, 128)
    owner = fast_owner.reshape(FAST // 128, 128)
    excl = exclusions.T
    f32 = jnp.float32
    vmem = pl.BlockSpec(memory_space=pltpu.VMEM)
    hbm = pl.BlockSpec(memory_space=pltpu.HBM)
    dma = pltpu.SemaphoreType.DMA
    outs = pl.pallas_call(
        kernel,
        out_shape=(
            jax.ShapeDtypeStruct((3, PIECE), f32),
            jax.ShapeDtypeStruct((3, PIECE), f32),
            jax.ShapeDtypeStruct((3, CELLS, CELL), f32),
            jax.ShapeDtypeStruct((3, CELLS, CELL), f32),
        ),
        in_specs=[hbm] * 9,
        out_specs=(vmem,) * 4,
        scratch_shapes=[
            pltpu.VMEM((3, PIECE), f32),
            pltpu.VMEM((3, PIECE), f32),
            pltpu.VMEM((FAST // 128, 128), f32),
            pltpu.VMEM((8, 128), jnp.int32),
            pltpu.VMEM((4, MOL), jnp.int32),
            pltpu.VMEM((3, CELLS, CELL), f32),
            pltpu.VMEM((3, CELLS, CELL), f32),
            pltpu.VMEM((CELLS, CELL), f32),
            pltpu.SMEM((NBR, CR, CC), jnp.int32),
            pltpu.VMEM((2, ROWS, 128), f32),
            dma((9,)),
            pltpu.VMEM((1, 128), f32),
            pltpu.VMEM((ROWS * COLS, 1, 128), f32),
            pltpu.VMEM((1, 128), f32),
            pltpu.VMEM((LINE, 1, 128), f32),
            pltpu.VMEM((INNER + 1, ROWS, 2, 4, 128), f32),
            pltpu.VMEM((3, 2, ROWS, 128), f32),
            pltpu.VMEM((ROWS, 2, 4, 128), f32),
            pltpu.VMEM((2 * ROWS, 4, 128), f32),
            pltpu.VMEM((4, 128), f32),
            pltpu.VMEM((LINE, 4, 128), f32),
            pltpu.VMEM((3, 128, 128), f32),
            pltpu.VMEM((3, 128, 128), f32),
            pltpu.VMEM((CR + 4, CC + 4, 4, CELL), f32),
            pltpu.VMEM((CR + 4, CC + 4, 4, CELL), f32),
            pltpu.VMEM((3, CELL, CELL), f32),
            pltpu.VMEM((3, CELL, CELL), f32),
            pltpu.VMEM((3, CELL, CELL), f32),
            pltpu.VMEM((3, CELL, CELL), f32),
            pltpu.VMEM((3, CELLS, CELL), f32),
            pltpu.VMEM((4 * CELL, MOL), f32),
            pltpu.VMEM((3, ROWS, MOL), f32),
            pltpu.VMEM((ROWS * COLS, 1, 128), f32),
            pltpu.VMEM((ROWS * COLS, 1, 128), f32),
            pltpu.VMEM((2, 2, 1, 128), f32),
            pltpu.VMEM((ROWS, 128), f32),
            dma,
            dma((2,)),
            dma,
            dma,
            dma((INNER + 1,)),
            dma((INNER + 1, ROWS)),
            dma,
            dma,
            dma,
            dma,
            dma((2, 8)),
            dma((2, 8)),
            dma,
            dma,
        ],
        compiler_params=pltpu.CompilerParams(
            collective_id=0, has_side_effects=True, vmem_limit_bytes=VMEM
        ),
    )(
        fast_pos,
        fast_vel,
        charge,
        owner,
        excl,
        slow_pos.reshape(3, CELLS, CELL),
        slow_vel.reshape(3, CELLS, CELL),
        slow_charge.reshape(CELLS, CELL),
        neighbours.transpose(2, 0, 1),
    )
    outs = pl.pallas_call(
        finish, out_shape=[jax.ShapeDtypeStruct(o.shape, f32) for o in outs], in_specs=[vmem] * 4, out_specs=[vmem] * 4,
        compiler_params=pltpu.CompilerParams(vmem_limit_bytes=VMEM),
    )(*outs)
    fpos, fvel, spos, svel = outs
    return fpos, fvel, spos.reshape(3, CR, CC, CELL), svel.reshape(3, CR, CC, CELL)


def solution(mesh):
    specs = (
        P(None, ("row", "col")),
        P(None, ("row", "col")),
        P(),
        P(),
        P(),
        P(None, "row", "col", None),
        P(None, "row", "col", None),
        P("row", "col", None),
        P("row", "col", None),
    )
    return jax.shard_map(
        per_device,
        mesh=mesh,
        in_specs=specs,
        out_specs=(specs[0], specs[1], specs[5], specs[6]),
        check_vma=False,
    )
```
